32 devices in a mesh: rep: 1 (over z), dp: 4 (over y), mp: 8 (over x, core).
Axes of the slice: x: 4, y: 4, z: 1, core: 2. Of those that a mesh axis runs over, the one named last changes fastest.
The devices are a block of a 4x4x8 slice.
Arguments:
- x: bfloat16 [4, 2048, 4096], P(('rep', 'dp'), 'mp')
- lengths: int32 [4], P(('rep', 'dp'))
- gamma: bfloat16 [2, 4096], P(None, 'dp')
- wq: bfloat16 [2, 4096, 4096], P(None, 'dp', 'mp')
- wkv: bfloat16 [2, 4096, 512], P(None, 'dp')
- wg: bfloat16 [2, 4096, 16384], P(None, 'dp', 'mp')
- wu: bfloat16 [2, 4096, 16384], P(None, 'dp', 'mp')
- wo: bfloat16 [2, 4096, 4096], P(None, 'mp', 'dp')
- wd: bfloat16 [2, 16384, 4096], P(None, 'mp', 'dp')
Outputs:
- output: bfloat16 [4, 2048, 4096], P(('rep', 'dp'), 'mp')
All inputs are finite; a program needn't handle non-finite values.
Results may differ from the reference program's by a relative error of at most 0.0178136.
Values are sent between devices in bfloat16 or wider.
A program may use at most 768 MiB of HBM per device.

```python
import math
import jax
import jax.numpy as jnp
from jax import lax

D = 4096
HEADS = 16
HEAD = 256
FF = 16384
BATCH = 4
SEQ = 2048

EPS = 1e-6
QBLK = math.gcd(SEQ, 128)


def setup_inputs(seed: int = 0, part: int = 0) -> dict:
    key = jax.random.key(seed)
    kpart, kshared = jax.random.split(key)
    kp = jax.random.fold_in(kpart, part)
    kx, kl = jax.random.split(kp)
    kw = jax.random.split(kshared, 7)
    x = jax.random.normal(kx, (BATCH, SEQ, D), jnp.float32).astype(jnp.bfloat16)
    kc, ks = jax.random.split(jax.random.fold_in(kl, 7))
    full = jax.random.bernoulli(kc, 0.4, (BATCH,))
    short = jax.random.randint(ks, (BATCH,), 1, SEQ + 1)
    lengths = jnp.where(full, SEQ, short).astype(jnp.int32)
    qk = 1.25 * D ** -0.5
    gamma = (1.0 + 0.3 * jax.random.normal(kw[0], (2, D), jnp.float32)).astype(jnp.bfloat16)
    wq = (jax.random.normal(kw[1], (2, D, HEADS * HEAD), jnp.float32) * qk).astype(jnp.bfloat16)
    wkv = (jax.random.normal(kw[2], (2, D, 2 * HEAD), jnp.float32) * qk).astype(jnp.bfloat16)
    wg = (jax.random.normal(kw[3], (2, D, FF), jnp.float32) * D ** -0.5).astype(jnp.bfloat16)
    wu = (jax.random.normal(kw[4], (2, D, FF), jnp.float32) * D ** -0.5).astype(jnp.bfloat16)
    wo = (jax.random.normal(kw[5], (2, HEADS * HEAD, D), jnp.float32) * (2.0 * (HEADS * HEAD) ** -0.5)).astype(jnp.bfloat16)
    wd = (jax.random.normal(kw[6], (2, FF, D), jnp.float32) * FF ** -0.5).astype(jnp.bfloat16)
    return {'x': x, 'lengths': lengths, 'gamma': gamma, 'wq': wq, 'wkv': wkv,
            'wg': wg, 'wu': wu, 'wo': wo, 'wd': wd}


def norm(x, g):
    xf = x.astype(jnp.float32)
    mu = jnp.mean(xf, axis=-1, keepdims=True)
    xc = xf - mu
    var = jnp.mean(xc * xc, axis=-1, keepdims=True)
    return (xc * lax.rsqrt(var + EPS) * g.astype(jnp.float32)).astype(jnp.bfloat16)


def attend(q, k, v, length):
    qs = q.reshape(SEQ // QBLK, QBLK, HEADS, HEAD).astype(jnp.float32)
    kf = k.astype(jnp.float32)
    vf = v.astype(jnp.float32)
    kpos = jnp.arange(SEQ)

    def blk(args):
        qi, start = args
        s = jnp.einsum('qhd,kd->hqk', qi, kf) * (HEAD ** -0.5)
        qpos = start + jnp.arange(QBLK)
        ok = (kpos[None, :] <= qpos[:, None]) & (kpos[None, :] < length)
        s = jnp.where(ok[None], s, -1e30)
        p = jax.nn.softmax(s, axis=-1).astype(jnp.bfloat16).astype(jnp.float32)
        return jnp.einsum('hqk,kd->qhd', p, vf).astype(jnp.bfloat16)

    o = lax.map(blk, (qs, jnp.arange(SEQ // QBLK) * QBLK))
    return o.reshape(SEQ, HEADS * HEAD)


def layer(x, lengths, g, wq, wkv, wg, wu, wo, wd):
    h = norm(x, g).reshape(BATCH * SEQ, D)
    q = jnp.dot(h, wq, preferred_element_type=jnp.float32).astype(jnp.bfloat16)
    kv = jnp.dot(h, wkv, preferred_element_type=jnp.float32).astype(jnp.bfloat16)
    gt = jnp.dot(h, wg, preferred_element_type=jnp.float32).astype(jnp.bfloat16)
    up = jnp.dot(h, wu, preferred_element_type=jnp.float32).astype(jnp.bfloat16)
    m = (jax.nn.silu(gt.astype(jnp.float32)) * up.astype(jnp.float32)).astype(jnp.bfloat16)
    q = q.reshape(BATCH, SEQ, HEADS, HEAD)
    kv = kv.reshape(BATCH, SEQ, 2 * HEAD)
    o = lax.map(lambda a: attend(a[0], a[1][:, :HEAD], a[1][:, HEAD:], a[2]), (q, kv, lengths))
    z = (jnp.dot(o.reshape(BATCH * SEQ, HEADS * HEAD), wo, preferred_element_type=jnp.float32)
         + jnp.dot(m, wd, preferred_element_type=jnp.float32))
    return (x.astype(jnp.float32) + z.reshape(BATCH, SEQ, D)).astype(jnp.bfloat16)


def reference(x, lengths, gamma, wq, wkv, wg, wu, wo, wd):
    def step(carry, w):
        return layer(carry, lengths, w[0], w[1], w[2], w[3], w[4], w[5], w[6]), None
    y, _ = lax.scan(step, x, (gamma, wq, wkv, wg, wu, wo, wd))
    return y
```

```python
import functools
import jax
import jax.numpy as jnp
from jax import lax
from jax.experimental import pallas as pl
from jax.experimental.pallas import tpu as pltpu
from jax.sharding import PartitionSpec as P

EPS = 1e-6
BF = jnp.bfloat16
F32 = jnp.float32
GROUPS = 2


SWAP_T = [(0, 3), (3, 0), (1, 2), (2, 1)]
SWAP_S = [(0, 1), (1, 0), (2, 3), (3, 2)]


def dot(a, b):
    return jnp.dot(a, b, preferred_element_type=F32)


def scope(name):
    return jax.named_scope(name)


def slot_dims(r):
    return jnp.stack([r, r ^ 1, 3 - r, r ^ 2]).astype(jnp.int32)


def params(**kw):
    return pltpu.CompilerParams(vmem_limit_bytes=60 * 2**20, **kw)


def ln_rows(xf, g):
    mu = jnp.mean(xf, axis=-1, keepdims=True)
    xc = xf - mu
    var = jnp.mean(xc * xc, axis=-1, keepdims=True)
    return (xc * lax.rsqrt(var + EPS) * g).astype(BF)


def ln_kernel(x_ref, g_ref, h_ref):
    h_ref[...] = ln_rows(x_ref[...].astype(F32), g_ref[...].astype(F32))


def ln(x, g):
    t, d = x.shape
    tm = min(t, 64)
    return pl.pallas_call(
        ln_kernel, out_shape=jax.ShapeDtypeStruct((t, d), BF), grid=(t // tm,),
        in_specs=[pl.BlockSpec((tm, d), lambda i: (i, 0)), pl.BlockSpec((1, d), lambda i: (0, 0))],
        out_specs=pl.BlockSpec((tm, d), lambda i: (i, 0)), compiler_params=params(),
        cost_estimate=pl.CostEstimate(flops=t * d * 10, bytes_accessed=t * d * 4, transcendentals=0),
        name="ln")(x, g)


def residual_kernel(last, dims, x_ref, z_ref, t_ref, g_ref, *outs):
    y_ref = outs[0]
    nb, _, w = z_ref.shape
    per = nb // 4
    for cb in range(nb):
        cols = pl.ds(pl.multiple_of((dims[cb // per] * per + cb % per) * w, w), w)
        z = z_ref[cb].astype(F32) + t_ref[(cb + 2 * per) % nb].astype(F32)
        y_ref[:, cols] = (x_ref[:, cols].astype(F32) + z).astype(BF)
    if not last:
        outs[1][...] = ln_rows(y_ref[...].astype(F32), g_ref[...].astype(F32))


def residual(x, z, zt, dims, g, last):
    t, d = x.shape
    nb, _, w = z.shape
    tm = min(t, 64)
    full = pl.BlockSpec((tm, d), lambda i, s: (i, 0))
    part = pl.BlockSpec((nb, tm, w), lambda i, s: (0, i, 0))
    n = 1 if last else 2
    out = pl.pallas_call(
        functools.partial(residual_kernel, last), out_shape=[jax.ShapeDtypeStruct((t, d), BF)] * n,
        grid_spec=pltpu.PrefetchScalarGridSpec(
            num_scalar_prefetch=1, grid=(t // tm,),
            in_specs=[full, part, part, pl.BlockSpec((1, d), lambda i, s: (0, 0))],
            out_specs=[full] * n),
        compiler_params=params(), name="residual")(dims, x, z, zt, g)
    return out[0], (None if last else out[1])


def slots_dot(h_ref, ws, dims):
    acc = None
    for d in range(4):
        q = ws[d].shape[0]
        part = dot(h_ref[:, pl.ds(pl.multiple_of(dims[d] * q, 128), q)], ws[d][...])
        acc = part if acc is None else acc + part
    return acc


def ff_kernel(dims, h_ref, *refs):
    ws, m_ref = refs[:4], refs[4]
    a = slots_dot(h_ref, ws, dims)
    n = m_ref.shape[1]
    gt = a[:, :n].astype(BF).astype(F32)
    up = a[:, n:].astype(BF).astype(F32)
    m_ref[...] = (gt * jax.nn.sigmoid(gt) * up).astype(BF)


def proj_kernel(dims, h_ref, *refs):
    refs[4][...] = slots_dot(h_ref, refs[:4], dims).astype(BF)


def slotted(kernel, h, ws, dims, n, name, tm=512):
    t, d = h.shape
    q, w = ws[0].shape
    return pl.pallas_call(
        kernel, out_shape=jax.ShapeDtypeStruct((t, n), BF),
        grid_spec=pltpu.PrefetchScalarGridSpec(
            num_scalar_prefetch=1, grid=(t // tm,),
            in_specs=[pl.BlockSpec((tm, d), lambda i, s: (i, 0))]
            + [pl.BlockSpec((q, w), lambda i, s: (0, 0), pipeline_mode=pl.Buffered(1))] * 4,
            out_specs=pl.BlockSpec((tm, n), lambda i, s: (i, 0))),
        compiler_params=params(),
        cost_estimate=pl.CostEstimate(flops=2 * t * d * w, bytes_accessed=2 * (t * d + d * w + t * n), transcendentals=t * n),
        name=name)(dims, h, *ws)


def kv_kernel(h_ref, w_ref, o_ref):
    o_ref[...] = dot(h_ref[...], w_ref[...]).astype(BF)


def kv_proj(h, w, tm=512):
    t, d = h.shape
    n = w.shape[1]
    return pl.pallas_call(
        kv_kernel, out_shape=jax.ShapeDtypeStruct((t, n), BF), grid=(t // tm,),
        in_specs=[pl.BlockSpec((tm, d), lambda i: (i, 0)),
                  pl.BlockSpec((d, n), lambda i: (0, 0), pipeline_mode=pl.Buffered(1))],
        out_specs=pl.BlockSpec((tm, n), lambda i: (i, 0)), compiler_params=params(),
        cost_estimate=pl.CostEstimate(flops=2 * t * d * n, bytes_accessed=2 * (t * d + d * n + t * n), transcendentals=0),
        name="kv")(h, w)


def attn_kernel(len_ref, q_ref, kv_ref, o_ref, s_ref):
    i = pl.program_id(0)
    bq, dh = q_ref.shape
    n = len_ref[0]
    q = q_ref[...]
    row = lax.broadcasted_iota(jnp.int32, (bq, bq), 0) + i * bq

    def score(j, m):
        at = pl.multiple_of(j * bq, bq)
        k = kv_ref[pl.ds(at, bq), :dh]
        s = lax.dot_general(q, k, (((1,), (1,)), ((), ())), preferred_element_type=F32) * (dh ** -0.5)
        col = lax.broadcasted_iota(jnp.int32, (bq, bq), 1) + j * bq
        s = jnp.where((col <= row) & (col < n), s, -1e30)
        s_ref[j] = s
        return jnp.maximum(m, jnp.max(s, axis=1, keepdims=True))

    m = lax.fori_loop(0, i + 1, score, jnp.full((bq, 1), -1e30, F32))

    def expo(j, l):
        p = jnp.exp(s_ref[j] - m)
        s_ref[j] = p
        return l + jnp.sum(p, axis=1, keepdims=True)

    l = lax.fori_loop(0, i + 1, expo, jnp.zeros((bq, 1), F32))

    def value(j, o):
        at = pl.multiple_of(j * bq, bq)
        return o + dot((s_ref[j] / l).astype(BF), kv_ref[pl.ds(at, bq), dh:])

    o = lax.fori_loop(0, i + 1, value, jnp.zeros((bq, dh), F32))
    o_ref[...] = o.astype(BF)


def attend(q, kv, length, bq=256):
    t, dh = q.shape
    return pl.pallas_call(
        attn_kernel, out_shape=jax.ShapeDtypeStruct((t, dh), BF),
        grid_spec=pltpu.PrefetchScalarGridSpec(
            num_scalar_prefetch=1, grid=(t // bq,),
            in_specs=[pl.BlockSpec((bq, dh), lambda i, s: (i, 0)),
                      pl.BlockSpec((t, 2 * dh), lambda i, s: (0, 0), pipeline_mode=pl.Buffered(1))],
            out_specs=pl.BlockSpec((bq, dh), lambda i, s: (i, 0)),
            scratch_shapes=[pltpu.VMEM((t // bq, bq, bq), F32)]),
        compiler_params=params(),
        cost_estimate=pl.CostEstimate(flops=4 * t * t * dh, bytes_accessed=8 * t * dh, transcendentals=t * t // 2),
        name="attn")(length, q, kv)


MESH = pl.DeviceIdType.MESH
CB = 512
RING, LAG = 4, 2


def reduce_kernel(chips, nslot, ngroup, *refs):
    n_in = 2 * (1 + ngroup) + nslot
    parts, ws = refs[:2 * (1 + ngroup)], refs[2 * (1 + ngroup):n_in]
    z_ref, zt_ref = refs[n_in:n_in + 2]
    (om, w, sl, rel, fin, sib, acc, in_sem, sib_s, sib_r, rel_s, rel_r, fin_s, fin_r, t_s, t_r) = refs[n_in + 2:]
    nb = z_ref.shape[0]
    rows = z_ref.shape[1]
    per = w.shape[2] // CB
    j = lax.axis_index('mp')
    r = lax.axis_index('dp')
    chip, core = j // 2, j % 2

    def at(off):
        return {'mp': lax.rem(chip + off, chips) * 2 + core}

    peers = [{'mp': chip * 2 + 1 - core}, at(1), at(chips - 1), {'dp': 3 - r}]
    barrier = pltpu.get_barrier_semaphore()
    for p in peers:
        pl.semaphore_signal(barrier, inc=1, device_id=p, device_id_type=MESH)

    loads = []
    for b in (1, 0):
        col = 0
        for k in range(1 + ngroup):
            src = parts[b * (1 + ngroup) + k]
            loads.append(pltpu.make_async_copy(src, om.at[b, :, pl.ds(col, src.shape[1])], in_sem.at[len(loads)]))
            col += src.shape[1]
    for d in range(nslot):
        loads.append(pltpu.make_async_copy(ws[d], w.at[d], in_sem.at[len(loads)]))
    for c in loads:
        c.start()
    pl.semaphore_wait(barrier, len(peers))
    for c in loads:
        c.wait()

    def rcopy(src, dst, s, q, dev):
        return pltpu.make_async_remote_copy(src_ref=src, dst_ref=dst, send_sem=s, recv_sem=q, device_id=dev, device_id_type=MESH)

    def sib_copy(st, b, cb):
        k = lax.rem(cb, RING)
        return rcopy(sib.at[k], sl.at[st, b, cb], sib_s.at[k], sib_r.at[st, b, cb], peers[0])

    def out_copy(st, b, cb):
        odd = lax.rem(cb, 2)
        src = sl.at[st, b, cb]
        if st == 0:
            return rcopy(src, rel.at[b, cb], rel_s.at[b, cb], rel_r.at[b, cb], at(1 + 2 * odd))
        if st == 1:
            p, off = 1 - odd, 3 - 2 * odd
        else:
            p, off = odd, 1 + 2 * odd
        return rcopy(src, fin.at[p, b, cb], fin_s.at[p, b, cb], fin_r.at[p, b, cb], at(off))

    def compute(st, b, cb):
        odd = lax.rem(cb, 2)
        off = (2, 3 - 2 * odd, 1 + 2 * odd, 0)[st]
        row = pl.multiple_of(lax.rem(chip + off, chips) * (2 * rows), 2 * rows)
        col = pl.multiple_of(lax.rem(cb, per) * CB, CB)
        a = acc.at[lax.rem(cb, LAG + 1)]
        a[...] = dot(om[b, pl.ds(row, 2 * rows), :], w[cb // per, :, pl.ds(col, CB)])

        @pl.when(cb >= RING)
        def _():
            sib_copy(st, b, cb - RING).wait_send()
        sib[lax.rem(cb, RING)] = a[pl.ds(pl.multiple_of((1 - core) * rows, rows), rows), :].astype(BF)
        sib_copy(st, b, cb).start()

    def combine(st, b, cb):
        sib_copy(st, b, cb).wait_recv()
        a = acc.at[lax.rem(cb, LAG + 1)]
        v = a[pl.ds(pl.multiple_of(core * rows, rows), rows), :] + sl[st, b, cb].astype(F32)
        if st == 2:
            out_copy(0, b, cb).wait_recv()
            v = v + rel[b, cb].astype(F32)
        sl[st, b, cb] = v.astype(BF)
        if st < 3:
            out_copy(st, b, cb).start()

    def stage(st, b):
        @pl.loop(0, nb)
        def _(cb):
            compute(st, b, cb)

            @pl.when(cb >= LAG)
            def _():
                combine(st, b, cb - LAG)

        @pl.loop(nb - LAG, nb)
        def _(cb):
            combine(st, b, cb)

        @pl.loop(max(0, nb - RING), nb)
        def _(cb):
            sib_copy(st, b, cb).wait_send()

    for st, b in ((0, 1), (0, 0), (1, 1), (2, 1), (1, 0), (2, 0), (3, 1), (3, 0)):
        stage(st, b)

    def t_copy(cb):
        return rcopy(sl.at[3, 1, cb], zt_ref.at[cb], t_s.at[cb], t_r.at[cb], peers[3])

    for b in (1, 0):
        @pl.loop(0, nb)
        def _(cb, b=b):
            odd = lax.rem(cb, 2)
            for p in range(2):
                pltpu.make_async_copy(fin.at[p, b, cb], fin.at[p, b, cb], fin_r.at[p, b, cb]).wait()
            v = sl[3, b, cb].astype(F32) + fin[0, b, cb].astype(F32) + fin[1, b, cb].astype(F32)
            if b == 0:
                z_ref[cb] = v.astype(BF)
            else:
                sl[3, 1, cb] = v.astype(BF)
                t_copy(cb).start()

    @pl.loop(0, nb)
    def _(cb):
        t_copy(cb).wait()
        for b in (1, 0):
            for st in range(3):
                out_copy(st, b, cb).wait_send()


def out_reduce(oms, ws, mesh, cid):
    t = oms[0][0].shape[0]
    k, width = ws[0].shape
    mp = mesh.shape['mp']
    rows, nslot, ngroup = t // mp, len(ws), len(oms[0][1])
    nb = nslot * width // CB
    unit = (rows, CB)
    dma = pltpu.SemaphoreType.DMA
    any_spec = pl.BlockSpec(memory_space=pl.ANY)
    args = [a for o, ms in oms for a in (o, *ms)] + list(ws)
    out = jax.ShapeDtypeStruct((nb, *unit), BF)
    return pl.pallas_call(
        functools.partial(reduce_kernel, mp // 2, nslot, ngroup),
        out_shape=[out, out],
        in_specs=[any_spec] * len(args),
        out_specs=[pl.BlockSpec(memory_space=pltpu.VMEM)] * 2,
        scratch_shapes=[
            pltpu.VMEM((2, t, k), BF), pltpu.VMEM((nslot, k, width), BF),
            pltpu.VMEM((4, 2, nb, *unit), BF), pltpu.VMEM((2, nb, *unit), BF), pltpu.VMEM((2, 2, nb, *unit), BF),
            pltpu.VMEM((RING, *unit), BF), pltpu.VMEM((LAG + 1, 2 * rows, CB), F32),
            dma((len(args),)), dma((RING,)), dma((4, 2, nb)), dma((2, nb)), dma((2, nb)), dma((2, 2, nb)), dma((2, 2, nb)),
            dma((nb,)), dma((nb,))],
        compiler_params=pltpu.CompilerParams(vmem_limit_bytes=63 * 2**20, collective_id=cid, has_side_effects=True),
        cost_estimate=pl.CostEstimate(flops=4 * t * k * nslot * width, bytes_accessed=2 * (2 * t * k + nslot * k * width), transcendentals=0),
        name="zred")(*args)


def piece(w, axis, i, n):
    size = w.shape[axis] // n
    return lax.dynamic_slice_in_dim(w, i * size, size, axis)


def bundles(wq, wg, wu, wo, wd, half):
    out = {"q": piece(wq, 1, half, 2)}
    for i in range(GROUPS):
        at = half * GROUPS + i
        out[f"g{i}"] = jnp.concatenate([piece(wg, 1, at, 2 * GROUPS), piece(wu, 1, at, 2 * GROUPS)], axis=1)
    out["o"] = jnp.concatenate([piece(wo, 0, half, 2), piece(wd, 0, half, 2)], axis=0)
    return out


def spread(l, name, own, other):
    with scope(f"S{l}{name}"):
        s = lax.ppermute(own, 'dp', SWAP_S)
    with scope(f"T{l}{name}"):
        t = lax.ppermute(other, 'dp', SWAP_T)
    with scope(f"F{l}{name}"):
        f = lax.ppermute(t, 'dp', SWAP_S)
    return [own, s, t, f]


def solution(mesh):
    assert mesh.shape['dp'] == 4

    def body(x, lengths, gamma, wq, wkv, wg, wu, wo, wd):
        layers = gamma.shape[0]
        r, j = lax.axis_index('dp'), lax.axis_index('mp')
        half = r // 2
        dims = slot_dims(r)
        x = x[0]
        with scope("gamma"):
            g = lax.all_gather(gamma, 'dp', axis=1, tiled=True)
        with scope("lenT"):
            lens = [lengths, lax.ppermute(lengths, 'dp', SWAP_T)]
        with scope("ln0"):
            h = ln(x, g[0:1])
        with scope("wkv"):
            n = wkv.shape[1] // mesh.shape['mp']
            kvw = lax.dynamic_slice_in_dim(wkv, j * n, n, 1)
            kvw = lax.all_gather(kvw, ('dp', 'mp'), axis=1, tiled=True)
        for l in range(layers):
            own = bundles(wq[l], wg[l], wu[l], wo[l], wd[l], half)
            oth = bundles(wq[l], wg[l], wu[l], wo[l], wd[l], 1 - half)
            w = {name: spread(l, name, own[name], oth[name]) for name in own}
            with scope(f"hT{l}"):
                hp = lax.ppermute(h, 'dp', SWAP_T)
            om = []
            for b, hb in enumerate((h, hp)):
                with scope(f"ag{l}{b}"):
                    hb = lax.all_gather(hb, 'mp', axis=0, tiled=True)
                with scope(f"q{l}{b}"):
                    q = slotted(proj_kernel, hb, w["q"], dims, w["q"][0].shape[1], "q")
                ms = []
                for i in range(GROUPS):
                    with scope(f"ff{l}{b}{i}"):
                        ws = w[f"g{i}"]
                        ms.append(slotted(ff_kernel, hb, ws, dims, ws[0].shape[1] // 2, "ff"))
                with scope(f"kv{l}{b}"):
                    kv = kv_proj(hb, kvw[l])
                with scope(f"at{l}{b}"):
                    o = attend(q, kv, lens[b])
                om.append((o, ms))
            with scope(f"zred{l}"):
                z, zt = out_reduce(om, w["o"], mesh, 1)
            with scope(f"res{l}"):
                last = l == layers - 1
                x, h = residual(x, z, zt, dims, g[l:l + 1] if last else g[l + 1:l + 2], last)
        return x[None]

    in_specs = (P(('rep', 'dp'), 'mp', None), P(('rep', 'dp')), P(None, 'dp'),
                P(None, 'dp', 'mp'), P(None, 'dp', None), P(None, 'dp', 'mp'),
                P(None, 'dp', 'mp'), P(None, 'mp', 'dp'), P(None, 'mp', 'dp'))
    return jax.shard_map(body, mesh=mesh, in_specs=in_specs,
                         out_specs=P(('rep', 'dp'), 'mp', None), check_vma=False)
```

```python
import functools
import jax
import jax.numpy as jnp
from jax import lax
from jax.experimental import pallas as pl
from jax.experimental.pallas import tpu as pltpu
from jax.sharding import PartitionSpec as P

EPS = 1e-6
BF = jnp.bfloat16
F32 = jnp.float32
MESH = pl.DeviceIdType.MESH
DMA = pltpu.SemaphoreType.DMA
ANY = pl.BlockSpec(memory_space=pl.ANY)
VM = pl.BlockSpec(memory_space=pltpu.VMEM)
NT = 4
CB = 512
RING, LAG = 4, 2
VMEM_LIMIT = 63 * 2**20

OWN, PART, MATE, FAR = SLOTS = range(4)
S, T, F = KINDS = range(3)
GATE, UP = GU = range(2)
MINE, THEIRS = SEQS = range(2)


def scope(name):
    return jax.named_scope(name)


def timed(name):
    def wrap(f):
        @functools.wraps(f)
        def g(*args):
            with scope("_".join([name, *(str(a) for a in args if isinstance(a, int))])):
                return f(*args)
        return g
    return wrap


def dot(a, b):
    return jnp.dot(a, b, preferred_element_type=F32)


def remote(src, dst, s, q, dev):
    return pltpu.make_async_remote_copy(src_ref=src, dst_ref=dst, send_sem=s, recv_sem=q, device_id=dev, device_id_type=MESH)


local = pltpu.make_async_copy


def span(i, n):
    return pl.ds(pl.multiple_of(i * n, n), n)


def each(lo, hi):
    return pl.loop(lo, hi)


class Place:
    def __init__(self, chips):
        self.chips = chips
        self.r = lax.axis_index('dp')
        self.j = lax.axis_index('mp')
        self.chip, self.core = self.j // 2, self.j % 2
        mate = self.r + 1 - 2 * (self.r % 2)
        self.slots = (self.r, 3 - self.r, mate, lax.rem(self.r + 2, 4))
        self.half = self.r // 2
        self.partner, self.mate, self.across = ({'dp': s} for s in self.slots[1:])
        self.sib = {'mp': self.chip * 2 + 1 - self.core}
        self.next, self.prev = self.at(1), self.at(chips - 1)

    def chip_at(self, off):
        return lax.rem(self.chip + off, self.chips)

    def at(self, off):
        return {'mp': self.chip_at(off) * 2 + self.core}

    def meet(self, *peers):
        barrier = pltpu.get_barrier_semaphore()
        for p in peers:
            pl.semaphore_signal(barrier, inc=1, device_id=p, device_id_type=MESH)
        pl.semaphore_wait(barrier, len(peers))


class Pieces:
    def __init__(self, layer, wq, wg, wu, me):
        self.layer, self.me = layer, me
        self.wq, self.w = wq, (wg, wu)
        self.nq = wq.shape[2] // 2
        self.nf = wg.shape[2] // 2
        self.tile = self.nf // NT

    def q(self, half):
        return self.wq.at[self.layer, :, span(half, self.nq)]

    def g(self, half, which, t):
        return self.w[which].at[self.layer, :, span(half * NT + t, self.tile)]

    def tile_part(self, buf, which):
        return buf.at[:, pl.ds(which * self.tile, self.tile)]


def out_rows(layer, half, wo, wd):
    return [w.at[layer, span(half, w.shape[1] // 2), :] for w in (wo, wd)]


def split_rows(o, n):
    return [o.at[pl.ds(0, n), :], o.at[pl.ds(n, o.shape[0] - n), :]]


def front_kernel(layer, chips, *refs):
    first = layer == 0
    it = iter(refs)
    take = lambda n: [next(it) for _ in range(n)]
    x, gam, lens, wq, wkv, wg, wu, wo, wd = take(9)
    if first:
        om, hbuf, s_o, t_o, wkvb, gb, lenb = take(7)
    else:
        wkvb, sq, sg, tq, tg, fq, fg = take(7)
        om, hbuf, s_o, t_o = take(4)
        gb, lenb = gam, lens
    (wqkv, wgu, hv, qkv, hown, hpar, wkvp, sc, ms, os, y_s, y_r, ld, o_s, o_r, kv_sem, hv_sem, ms_sem, os_sem, ag_s, ag_r, own_sem,
     ex_s, ex_r) = it
    me = Place(chips)
    pc = Pieces(layer, wq, wg, wu, me)
    mp = 2 * chips
    tok, d4, nq = x.shape[0], wq.shape[1], pc.nq
    dh = nq

    def at_slot(s, which, t):
        if which < GATE:
            return wqkv.at[s, :, pl.ds(0, nq)]
        return pc.tile_part(wgu.at[s, t], which)

    def raw(half, which, t):
        return pc.q(half) if which < GATE else pc.g(half, which, t)

    def given(q, g, which, t):
        return q if which < GATE else pc.tile_part(g.at[t], which)

    def sem(which, t):
        return 0 if which < GATE else 1 + 2 * t + which

    def load(s, which, t):
        n = sem(which, t)
        if s == OWN:
            src = raw(me.half, which, t)
        else:
            src = given(*{MATE: (sq, sg), PART: (tq, tg), FAR: (fq, fg)}[s] if not first else (), which, t)
        return local(src, at_slot(s, which, t), ld.at[s, n])

    def move(kind, which, t):
        n = sem(which, t)
        if kind == S:
            return remote(raw(me.half, which, t), at_slot(MATE, which, t), y_s.at[S, n], y_r.at[S, n], me.mate)
        if kind == T:
            return remote(raw(1 - me.half, which, t), at_slot(PART, which, t), y_s.at[T, n], y_r.at[T, n], me.partner)
        src = at_slot(PART, which, t) if first else given(tq, tg, which, t)
        return remote(src, at_slot(FAR, which, t), y_s.at[F, n], y_r.at[F, n], me.mate)

    def parts(t):
        return [(GATE - 1, 0)] if t is None else [(w, t) for w in GU]

    def send(kind, *ts):
        for t in ts:
            for p in parts(t):
                move(kind, *p).start()

    @timed('relay')
    def relay(*ts):
        for t in ts:
            for p in parts(t):
                if first:
                    move(T, *p).wait_recv()
                move(F, *p).start()

    def sent_ahead(t):
        return not first and (t is None or (isinstance(t, int) and t < AHEAD))

    @timed('have')
    def have(*ts):
        for t in ts:
            for p in parts(t):
                load(OWN, *p).wait()
                if sent_ahead(t):
                    load(MATE, *p).wait()
                    load(FAR, *p).wait()
                else:
                    move(S, *p).wait_recv()
                    move(F, *p).wait_recv()
                if not first:
                    load(PART, *p).wait()

    every = [None, *range(NT)]
    for t in every:
        for p in parts(t):
            load(OWN, *p).start()
            if not first:
                load(PART, *p).start()
            if sent_ahead(t):
                load(MATE, *p).start()
                load(FAR, *p).start()

    with scope('meet'):
        me.meet(me.sib, me.next, me.prev, me.mate, me.partner, *([me.across] if first else []))

    own_o, oth_o = out_rows(layer, me.half, wo, wd), out_rows(layer, 1 - me.half, wo, wd)
    no = wo.shape[1] // 2
    ahead_o = zip(oth_o + [own_o[0], own_o[1].at[pl.ds(0, s_o.shape[0] - no), :]], split_rows(t_o, no) + split_rows(s_o, no),
                  [me.partner, me.partner, me.mate, me.mate])
    out_moves = [remote(src, dst, o_s.at[n], o_r.at[n], dev) for n, (src, dst, dev) in enumerate(ahead_o)]

    small = []
    if first:
        kv_own = local(wkv.at[:, span(me.j, wkv.shape[1] // mp), :], wkvp.at[:, OWN], own_sem.at[4])
        kv_own.start()
        for s, dev in ((PART, me.partner), (MATE, me.mate), (FAR, me.across)):
            small.append(remote(gam, gb.at[s], ex_s.at[s], ex_r.at[s], dev))
        small.append(remote(lens, lenb.at[THEIRS], ex_s.at[OWN], ex_r.at[OWN], me.partner))
        for c in small:
            c.start()
        gb[OWN] = gam[:, :]
        lenb[MINE] = lens[:, :]
        kv_own.wait()

        def kv_move(kind):
            src, dst, dev = ((OWN, MATE, me.mate), (OWN, PART, me.partner), (PART, FAR, me.mate))[kind]
            return remote(wkvp.at[:, src], wkvp.at[:, dst], ex_s.at[4 + kind], ex_r.at[4 + kind], dev)
        for k in (T, S):
            kv_move(k).start()
            send(k, None)
        send(T, 0)
        with scope('small'):
            for c in small:
                c.wait_recv()
    else:
        for t in range(1, NT):
            send(S, t)
            relay(t)

    @timed('norm')
    def norm():
        rb = 32

        @each(0, tok // rb)
        def _(i):
            rows = span(i, rb)
            xf = x[rows, :].astype(F32)
            mu = jnp.mean(xf, axis=-1, keepdims=True)
            xc = xf - mu
            rstd = lax.rsqrt(jnp.mean(xc * xc, axis=-1, keepdims=True) + EPS)
            for s in SLOTS:
                cols = span(me.slots[s], d4)
                hown[rows, cols] = ((x[rows, cols].astype(F32) - mu) * rstd * gb[s, layer:layer + 1, :]).astype(BF)
    norm()

    SIB, TO, SHARE, PASS, LAST = range(5)

    def gather(g, src, block, part):
        offs = (chips - 1, 1)
        dirs = (me.next, me.prev)

        def idx(off):
            return me.chip_at(off) * 2 + me.core

        def c(kind, k, h):
            n = 4 * kind + 2 * k + h
            sems = (ag_s.at[g, n], ag_r.at[g, n])
            if kind == SIB:
                return remote(src, block(me.j), *sems, me.sib)
            if kind == TO:
                return remote(part(src, h), part(block(me.j), h), *sems, dirs[k])
            b = part(block(idx(2 if kind == LAST else offs[k])), h)
            return remote(b, b, *sems, dirs[k] if kind == PASS else me.sib)

        mine = local(src, block(me.j), own_sem.at[g])
        tag = 'abvw'[g]

        class G:
            @timed('own' + tag)
            def own():
                for h in range(2):
                    for k in range(2):
                        c(TO, k, k ^ h).start()
                c(SIB, 0, 0).start()
                mine.start()

            @timed('near' + tag)
            def near():
                for h in range(2):
                    for k in range(2):
                        c(TO, k, k ^ h).wait_recv()
                        if h == 0:
                            c(PASS, k, k).start()
                        c(SHARE, k, k ^ h).start()

            @timed('far' + tag)
            def far():
                for k in range(2):
                    c(PASS, k, k).wait_recv()
                    c(LAST, k, k).start()

            @timed('has' + tag)
            def has(kind):
                if kind == SIB:
                    mine.wait()
                    c(SIB, 0, 0).wait_recv()
                for k in range(2):
                    if kind == LAST:
                        c(kind, k, k).wait_recv()
                    if kind == SHARE:
                        for h in range(2):
                            c(kind, k, k ^ h).wait_recv()

            def end():
                c(SIB, 0, 0).wait_send()
                for k in range(2):
                    for h in range(2):
                        c(TO, k, h).wait_send()
                        c(SHARE, k, h).wait_send()
                    c(PASS, k, k).wait_send()
                    c(LAST, k, k).wait_send()
        return G

    def h_block(b):
        return lambda j: hbuf.at[b, span(j, tok), :]

    def h_part(ref, k):
        return ref.at[pl.ds(k * (tok // 2), tok // 2), :]

    ga, gb2 = gather(0, hown, h_block(MINE), h_part), gather(1, hpar, h_block(THEIRS), h_part)
    ht = remote(hown, hpar, ex_s.at[7], ex_r.at[7], me.partner)

    rows2 = 2 * tok

    def chip_rows(i):
        return span(me.chip_at(i + i // 2 - 2 * (i // 3)), rows2)

    def hload(i):
        return local(hbuf.at[i // 4, chip_rows(lax.rem(i, 4)), :], hv.at[lax.rem(i, 2)], hv_sem.at[lax.rem(i, 2)])

    def hdot(buf, w):
        acc = None
        for s in SLOTS:
            p = dot(hv[buf, :, span(me.slots[s], d4)], w(s))
            acc = p if acc is None else acc + p
        return acc

    def mcopy(i, t, k):
        w = pc.tile
        return local(ms.at[k], om.at[i // 4, chip_rows(lax.rem(i, 4)), pl.ds(pl.multiple_of(nq + t * w, w), w)], ms_sem.at[k])

    def tile(i, t, m):
        k = lax.rem(m, 2)
        a = hdot(lax.rem(i, 2), lambda s: wgu[s, t])

        @pl.when(m >= 2)
        def _():
            mcopy(i, t, k).wait()
        gt = a[:, :pc.tile].astype(BF).astype(F32)
        up = a[:, pc.tile:].astype(BF).astype(F32)
        ms[k] = (gt * jax.nn.sigmoid(gt) * up).astype(BF)
        mcopy(i, t, k).start()

    def drain():
        for k in range(2):
            mcopy(0, 0, k).wait()

    def any_of(i, marks):
        return functools.reduce(lambda a, b: a | b, [i == g for g in marks])

    def sweep(b, nt, gates, hooks):
        lo = b * chips
        marks = [n for n in gates]

        @each(lo, lo + chips)
        def _(i):
            for g, f in gates.items():
                pl.when(i == g)(f)

            @pl.when(any_of(i, [lo, *marks]))
            def _():
                hload(i).start()

            @pl.when(jnp.logical_not(any_of(i + 1, [lo + chips, *marks])))
            def _():
                hload(i + 1).start()
            hload(i).wait()
            qkv[b, chip_rows(i - lo), :] = hdot(lax.rem(i, 2), lambda s: wqkv[s]).astype(BF)

            @each(0, nt)
            def _(t):
                for n, f in hooks.items():
                    pl.when((i == lo) & (b == MINE) & (t == n))(f)
                tile(i, t, (i - lo) * nt + t)
        drain()

    def late(lo_t, hi_t, lo, hi):
        n = hi - lo
        hload(lo).start()

        @each(0, n * (hi_t - lo_t))
        def _(u):
            i, t = lo + lax.rem(u, n), lo_t + u // n

            @pl.when(lax.rem(u, n) == 0)
            def _():
                have(t)

            @pl.when(u + 1 < n * (hi_t - lo_t))
            def _():
                hload(lo + lax.rem(u + 1, n)).start()
            hload(i).wait()
            tile(i, t, u)
        drain()

    bq, bk = sc.shape[1:]

    @timed('attend')
    def attend(b):
        nblk = qkv.shape[1] // bq
        ratio = bk // bq

        def ocp(i, k):
            return local(os.at[k], om.at[b, span(i, bq), pl.ds(0, dh)], os_sem.at[k])

        def lanes(a, op):
            w = a.shape[1] // ratio // 2
            return functools.reduce(op, [a[:, n * w:(n + 1) * w] for n in range(2 * ratio)])

        @each(0, nblk)
        def _(i):
            q = qkv[b, span(i, bq), pl.ds(0, dh)]
            length = lenb[b, :, :][:1, :1]
            colf = lax.broadcasted_iota(jnp.int32, (1, bk), 1).astype(F32)

            def raw_score(j):
                k = qkv[b, span(j, bk), pl.ds(dh, dh)]
                s = lax.dot_general(q, k, (((1,), (1,)), ((), ())), preferred_element_type=F32) * (dh ** -0.5)
                pos = jnp.broadcast_to(colf + (j * bk).astype(F32), (bq, bk))
                return jnp.where(pos < length, s, -1e30)

            def score(j, m):
                s = raw_score(j)
                sc[j] = s
                return jnp.maximum(m, lanes(s, jnp.maximum))

            last = i // ratio
            row = lax.broadcasted_iota(jnp.int32, (bq, bk), 0) + (i - last * ratio) * bq
            col = lax.broadcasted_iota(jnp.int32, (bq, bk), 1)
            s = jnp.where(col <= row, raw_score(last), -1e30)
            sc[last] = s
            m = jnp.max(lax.fori_loop(0, last, score, lanes(s, jnp.maximum)), axis=1, keepdims=True)

            def expo(j, l):
                p = jnp.exp(sc[j] - m)
                sc[j] = p
                return l + lanes(p, jnp.add)

            l = jnp.sum(lax.fori_loop(0, last + 1, expo, jnp.zeros((bq, bk // ratio // 2), F32)), axis=1, keepdims=True)
            inv = 1.0 / l

            def value(j, o):
                return o + dot((sc[j] * inv).astype(BF), qkv[b, span(j, bk), pl.ds(2 * dh, dh)])

            o = lax.fori_loop(0, last + 1, value, jnp.zeros((bq, dh), F32))
            k = lax.rem(i, 2)

            @pl.when(i >= 2)
            def _():
                ocp(i, k).wait()
            os[k] = o.astype(BF)
            ocp(i, k).start()
        for k in range(2):
            ocp(k, k).wait()

    def kv_load(u):
        s, j = u // mp, lax.rem(u, mp)
        return local(wkvb.at[layer, j, s], wqkv.at[s, span(j, wkvp.shape[2]), pl.ds(nq, 2 * dh)], kv_sem.at[u])

    def kv_loads(go):
        @each(0, 4 * mp)
        def _(u):
            go(kv_load(u))

    def near_of(g):
        def f():
            g.near()
            g.has(SHARE)
        return f

    def far_of(g):
        def f():
            g.far()
            g.has(LAST)
        return f

    def both(*fs):
        def f():
            for g in fs:
                g()
        return f

    def start_b():
        with scope('ht'):
            ht.wait_recv()
        gb2.own()

    ga.own()
    ht.start()
    if first:
        with scope('kvmove'):
            kv_move(T).wait_recv()
            kv_move(F).start()
            kv_move(S).wait_recv()
        send(S, 0)
        send(T, 1)
        relay(None)
        send(S, 1)
        with scope('kvmove2'):
            kv_move(F).wait_recv()
        gw = [gather(2 + n, wkvp.at[n], lambda j, n=n: wkvb.at[n, j], lambda ref, k: ref.at[pl.ds(2 * k, 2)]) for n in range(2)]
        relay(0)
        send(S, 2)
        send(T, 2)
        send(T, 3)
        ga.near()
        gw[0].own()
        for c in out_moves[:2]:
            c.start()
        ga.far()
        gw[0].near()
        start_b()
        gw[0].far()
        gw[1].own()
        for kind in (SIB, SHARE, LAST):
            gw[0].has(kind)
        kv_loads(lambda c: c.start())
        for kind in (SIB, SHARE, LAST):
            ga.has(kind)
        kv_loads(lambda c: c.wait())
        have(None, 0)

        @each(0, 2)
        def _(b):
            with scope('sweep'):
                sweep(b, 1, {chips: both(lambda: gb2.has(SIB), gb2.near), chips + 1: both(lambda: gb2.has(SHARE), gw[1].near),
                             chips + 3: both(far_of(gb2), gw[1].far)}, {})

            @pl.when(b == MINE)
            def _():
                relay(1)
                send(S, 3)
            attend(b)

            @pl.when(b == MINE)
            def _():
                relay(2)

            @pl.when(b == THEIRS)
            def _():
                relay(3)
                for c in out_moves[2:]:
                    c.start()
        with scope('late'):
            late(1, NT, 0, 2 * chips)
        for kind in (SIB, SHARE, LAST):
            gw[1].has(kind)
    else:
        for c in out_moves:
            c.start()
        kv_loads(lambda c: c.start())
        kv_loads(lambda c: c.wait())
        have(None, 0)

        @each(0, 2)
        def _(b):
            with scope('sweep'):
                sweep(b, 2 + b, {0: lambda: ga.has(SIB), 1: both(near_of(ga), start_b), 3: far_of(ga),
                                 chips: both(lambda: gb2.has(SIB), gb2.near), chips + 1: lambda: gb2.has(SHARE), chips + 3: far_of(gb2)},
                      {1: lambda: have(1)})
            attend(b)

            @pl.when(b == MINE)
            def _():
                with scope('late2'):
                    late(2, 3, 0, chips)
        with scope('late'):
            late(3, NT, 0, 2 * chips)

    with scope('end'):
        for t in every:
            for p in parts(t):
                if not sent_ahead(t):
                    move(S, *p).wait_send()
                    move(F, *p).wait_send()
                if first:
                    move(T, *p).wait_send()
        for c in out_moves:
            c.wait()
        ht.wait_send()
        ga.end()
        gb2.end()
        for c in small:
            c.wait_send()
        if first:
            gw[0].end()
            gw[1].end()
            for k in KINDS:
                kv_move(k).wait_send()


AHEAD = 1


def front(layer, mesh, x, gam, lens, weights, given):
    wq, wkv, wg, wu, wo, wd = weights
    tok, d = x.shape
    mp = mesh.shape['mp']
    chips = mp // 2
    first = layer == 0
    d4 = wq.shape[1]
    nq, nkv, nf = wq.shape[2] // 2, wkv.shape[2], wg.shape[2] // 2
    no, nd = wo.shape[1] // 2, wd.shape[1] // 2
    t = tok * mp
    kvr = wkv.shape[1] // mp
    sds = jax.ShapeDtypeStruct
    outs = [sds((2, t, nq + nf), BF), sds((2, t, d), BF), sds((no + nd // 2, d4), BF), sds((no + nd, d4), BF)]
    specs = [ANY] * 4
    if first:
        outs += [sds((2, mp, 4, kvr, nkv), BF), sds((4, *gam.shape), F32), sds((2, *lens.shape), F32)]
        specs += [ANY, VM, VM]
    npiece = 1 + 2 * NT
    return pl.pallas_call(
        functools.partial(front_kernel, layer, chips), out_shape=outs,
        in_specs=[VM, VM, VM] + [ANY] * (6 + len(given)), out_specs=specs,
        scratch_shapes=[
            pltpu.VMEM((4, d4, nq + nkv), BF), pltpu.VMEM((4, NT, d4, 2 * nf // NT), BF), pltpu.VMEM((2, 2 * tok, d), BF),
            pltpu.VMEM((2, t, nq + nkv), BF), pltpu.VMEM((tok, d), BF), pltpu.VMEM((tok, d), BF),
            pltpu.VMEM((2, 4, kvr, nkv), BF), pltpu.VMEM((t // nq // 2, nq, 2 * nq), F32),
            pltpu.VMEM((2, 2 * tok, nf // NT), BF), pltpu.VMEM((2, nq, nq), BF),
            DMA((3, npiece)), DMA((3, npiece)), DMA((4, npiece)), DMA((4,)), DMA((4,)), DMA((4 * mp,)), DMA((2,)), DMA((2,)), DMA((2,)),
            DMA((4, 20)), DMA((4, 20)), DMA((5,)), DMA((8,)), DMA((8,))],
        compiler_params=pltpu.CompilerParams(vmem_limit_bytes=VMEM_LIMIT, collective_id=2 * layer, has_side_effects=True),
        cost_estimate=pl.CostEstimate(flops=4 * t * d * (nq + nkv + 2 * nf), bytes_accessed=12 * t * d, transcendentals=0),
        name=f"front{layer}")(x, gam, lens, *weights, *given)


def back_kernel(layer, chips, nxt, *refs):
    it = iter(refs)
    take = lambda n: [next(it) for _ in range(n)]
    x, om_h, s_o, t_o, wo, wd = take(6)
    if nxt:
        wq, wg, wu = take(3)
    y = next(it)
    if nxt:
        sq, sg, tq, tg, fq, fg = take(6)
    (om, w, sl, rel, fin, zt, sib, acc, in_sem, w_s, w_r, p_s, p_r, sib_s, sib_r, rel_s, rel_r, fin_s, fin_r, t_s, t_r) = it
    me = Place(chips)
    nb, rows = zt.shape[:2]
    per = w.shape[2] // CB
    no, ns = wo.shape[1] // 2, s_o.shape[0]

    own_o = out_rows(layer, me.half, wo, wd)
    own_rows, mate_rows = split_rows(w.at[OWN], no), split_rows(w.at[MATE], ns)
    loads = [local(om_h.at[THEIRS], om.at[THEIRS], in_sem.at[0]), local(own_o[0], own_rows[0], in_sem.at[1]),
             local(own_o[1], own_rows[1], in_sem.at[2]), local(t_o, w.at[PART], in_sem.at[3]), local(om_h.at[MINE], om.at[MINE], in_sem.at[4]),
             local(s_o, mate_rows[0], in_sem.at[5])]
    for c in loads:
        c.start()
    me.meet(me.sib, me.next, me.prev, me.mate, me.partner)
    to_mate = [remote(own_o[1].at[pl.ds(ns - no, no + own_o[1].shape[0] - ns), :], mate_rows[1], w_s.at[0], w_r.at[0], me.mate), remote(t_o, w.at[FAR], w_s.at[1], w_r.at[1], me.mate)]
    for c in to_mate:
        c.start()
    passing = []
    if nxt:
        pc = Pieces(layer + 1, wq, wg, wu, me)

        def buffers(q, g, nt):
            return [q] + [pc.tile_part(g.at[t], which) for t in range(nt) for which in GU]

        def args(half, nt):
            return [pc.q(half)] + [pc.g(half, which, t) for t in range(nt) for which in GU]

        def ahead(kind, srcs, dsts, dev):
            return [remote(*sd, p_s.at[kind, n], p_r.at[kind, n], dev) for n, sd in enumerate(zip(srcs, dsts))]
        to_s = ahead(S, args(me.half, AHEAD), buffers(sq, sg, AHEAD), me.mate)
        to_t = ahead(T, args(1 - me.half, NT), buffers(tq, tg, NT), me.partner)
        on = ahead(F, buffers(tq, tg, AHEAD), buffers(fq, fg, AHEAD), me.mate)
        for c in to_t + to_s:
            c.start()
        passing = to_s + on + to_t[len(on):]
    with scope('loads'):
        for c in loads[:4]:
            c.wait()

    AWAY, NEAR, JOIN, HOME = range(4)

    def sib_copy(st, b, cb, m):
        k = lax.rem(m, RING)
        return remote(sib.at[k], sl.at[st, b, cb], sib_s.at[k], sib_r.at[st, b, cb], me.sib)

    def away_copy(b, cb):
        return remote(sl.at[AWAY, b, cb], rel.at[b, cb], rel_s.at[b, cb], rel_r.at[b, cb], me.at(1 + 2 * lax.rem(cb, 2)))

    def near_copy(st, b, cb):
        p = lax.rem(st + cb, 2)
        return remote(sl.at[st, b, cb], fin.at[p, b, cb], fin_s.at[p, b, cb], fin_r.at[p, b, cb], me.at(1 + 2 * p))

    def compute(off, st, b, cb, m):
        a = acc.at[lax.rem(m, LAG + 1)]
        a[:, :] = dot(om[b, span(me.chip_at(off), 2 * rows), :], w[cb // per, :, span(lax.rem(cb, per), CB)])

        @pl.when(m >= RING)
        def _():
            sib_copy(st, b, cb, m).wait_send()
        sib[lax.rem(m, RING)] = a[span(1 - me.core, rows), :].astype(BF)
        sib_copy(st, b, cb, m).start()

    def combined(st, b, cb, m):
        sib_copy(st, b, cb, m).wait_recv()
        a = acc.at[lax.rem(m, LAG + 1)]
        return a[span(me.core, rows), :] + sl[st, b, cb].astype(F32)

    def run(n, unit, off, finish):
        @each(0, n + LAG)
        def _(m):
            @pl.when(m < n)
            def _():
                st, b, cb = unit(m)
                compute(off(st, cb), st, b, cb, m)

            @pl.when(m >= LAG)
            def _():
                st, b, cb = unit(m - LAG)
                finish(st, b, cb, combined(st, b, cb, m - LAG))

        for m in range(RING):
            sib_copy(HOME, MINE, 0, m).wait_send()

    @timed('stages')
    def stages(lo, n):
        def away(m):
            return AWAY, 1 - m // n, lo + lax.rem(m, n)

        def away_on(st, b, cb, v):
            sl[st, b, cb] = v.astype(BF)
            away_copy(b, cb).start()
        run(2 * n, away, lambda st, cb: 2, away_on)

        def near(m):
            return NEAR + lax.rem(m // n, 2), 1 - m // (2 * n), lo + lax.rem(m, n)

        def near_on(st, b, cb, v):
            @pl.when(st == NEAR)
            def _():
                sl[st, b, cb] = v.astype(BF)

            @pl.when(st == JOIN)
            def _():
                away_copy(b, cb).wait_recv()
                sl[st, b, cb] = (v + rel[b, cb].astype(F32)).astype(BF)
            near_copy(st, b, cb).start()
        run(4 * n, near, lambda st, cb: 1 + 2 * lax.rem(st + cb, 2), near_on)

        def home(m):
            return HOME, 1 - m // n, lo + lax.rem(m, n)

        def home_on(st, b, cb, v):
            sl[st, b, cb] = v.astype(BF)
        run(2 * n, home, lambda st, cb: 0, home_on)

    def t_copy(cb):
        return remote(sl.at[HOME, THEIRS, cb], zt.at[cb], t_s.at[cb], t_r.at[cb], me.partner)

    def total(b, cb):
        for p in range(2):
            local(fin.at[p, b, cb], fin.at[p, b, cb], fin_r.at[p, b, cb]).wait()
        return sl[HOME, b, cb].astype(F32) + fin[0, b, cb].astype(F32) + fin[1, b, cb].astype(F32)

    @timed('theirs')
    def theirs(lo, hi):
        @each(lo, hi)
        def _(cb):
            sl[HOME, THEIRS, cb] = total(THEIRS, cb).astype(BF)
            t_copy(cb).start()

    def swapped(cb):
        slot = cb // per
        return (slot + 1 - 2 * (slot % 2)) * per + cb % per

    @timed('mine')
    def mine(slot):
        @each(0, per)
        def _(n):
            cb = slot * per + n
            z = total(MINE, cb)
            t_copy(swapped(cb)).wait_recv()
            cols = span(me.slots[slot] * per + n, CB)
            y[:, cols] = (x[:, cols].astype(F32) + (z.astype(BF).astype(F32) + zt[swapped(cb)].astype(F32))).astype(BF)

    @each(0, 3)
    def _(g):
        later = (g + 1) // 2
        lo, n = 2 * (g + later), 2 * (2 - later)

        @pl.when(g == 0)
        def _():
            loads[4].wait()
            loads[5].wait()
        for k in range(2):
            @pl.when(g == 1 + k)
            def _(k=k):
                with scope('w%d' % k):
                    to_mate[k].wait_recv()
        stages(lo, n)
        if nxt:
            @pl.when(g == 0)
            def _():
                with scope('passing'):
                    for t, f in zip(to_t, on):
                        t.wait_recv()
                        f.start()
        theirs(lo, lo + n)
    for slot in SLOTS:
        mine(slot)

    with scope('end'):
        @each(0, nb)
        def _(cb):
            t_copy(cb).wait_send()
            for b in SEQS:
                away_copy(b, cb).wait_send()
                for st in (NEAR, JOIN):
                    near_copy(st, b, cb).wait_send()
        for c in to_mate:
            c.wait_send()
        for c in passing:
            c.wait()
        if nxt:
            for c in to_t[:len(on)]:
                c.wait_send()


def back(layer, mesh, x, om, s_o, t_o, weights, last):
    wq, wkv, wg, wu, wo, wd = weights
    mp = mesh.shape['mp']
    tok, d = x.shape
    t, k = om.shape[1:]
    d4 = wo.shape[2]
    nb = d // CB
    unit = (tok, CB)
    nq, nf = wq.shape[2] // 2, wg.shape[2] // 2
    sds = jax.ShapeDtypeStruct
    outs, specs = [sds((tok, d), BF)], [VM]
    args = [x, om, s_o, t_o, wo, wd]
    if not last:
        args += [wq, wg, wu]
        for n in (AHEAD, NT, AHEAD):
            outs += [sds((d4, nq), BF), sds((n, d4, 2 * nf // NT), BF)]
        specs += [ANY] * 6
    npiece = 1 + 2 * NT
    return pl.pallas_call(
        functools.partial(back_kernel, layer, mp // 2, not last), out_shape=outs,
        in_specs=[VM] + [ANY] * (len(args) - 1), out_specs=specs,
        scratch_shapes=[
            pltpu.VMEM((2, t, k), BF), pltpu.VMEM((4, k, d4), BF),
            pltpu.VMEM((4, 2, nb, *unit), BF), pltpu.VMEM((2, nb, *unit), BF), pltpu.VMEM((2, 2, nb, *unit), BF), pltpu.VMEM((nb, *unit), BF),
            pltpu.VMEM((RING, *unit), BF), pltpu.VMEM((LAG + 1, 2 * tok, CB), F32),
            DMA((6,)), DMA((2,)), DMA((2,)), DMA((3, npiece)), DMA((3, npiece)), DMA((RING,)), DMA((4, 2, nb)),
            DMA((2, nb)), DMA((2, nb)), DMA((2, 2, nb)), DMA((2, 2, nb)), DMA((nb,)), DMA((nb,))],
        compiler_params=pltpu.CompilerParams(vmem_limit_bytes=VMEM_LIMIT, collective_id=2 * layer + 1, has_side_effects=True),
        cost_estimate=pl.CostEstimate(flops=4 * t * k * d, bytes_accessed=2 * (2 * t * k + 4 * k * d4), transcendentals=0),
        name=f"back{layer}")(*args)


def solution(mesh):
    assert mesh.shape['dp'] == len(SLOTS)

    def body(x, lengths, gamma, *weights):
        layers = gamma.shape[0]
        assert layers == 2
        x = x[0]
        gam = jnp.zeros((8, gamma.shape[1]), F32).at[:layers].set(gamma.astype(F32))
        lens = jnp.broadcast_to(lengths.astype(F32)[:, None], (8, 128))
        om, _, s_o, t_o, wkvb, gam, lens = front(0, mesh, x, gam, lens, weights, ())
        x, *ahead = back(0, mesh, x, om, s_o, t_o, weights, False)
        om, _, s_o, t_o = front(1, mesh, x, gam, lens, weights, (wkvb, *ahead))
        (x,) = back(1, mesh, x, om, s_o, t_o, weights, True)
        return x[None]

    in_specs = (P(('rep', 'dp'), 'mp', None), P(('rep', 'dp')), P(None, 'dp'),
                P(None, 'dp', 'mp'), P(None, 'dp', None), P(None, 'dp', 'mp'),
                P(None, 'dp', 'mp'), P(None, 'mp', 'dp'), P(None, 'mp', 'dp'))
    return jax.shard_map(body, mesh=mesh, in_specs=in_specs,
                         out_specs=P(('rep', 'dp'), 'mp', None), check_vma=False)
```

```python
import functools
import jax
import jax.numpy as jnp
from jax import lax
from jax.experimental import pallas as pl
from jax.experimental.pallas import tpu as pltpu
from jax.sharding import PartitionSpec as P

EPS = 1e-6
BF = jnp.bfloat16
F32 = jnp.float32
MESH = pl.DeviceIdType.MESH
DMA = pltpu.SemaphoreType.DMA
ANY = pl.BlockSpec(memory_space=pl.ANY)
VM = pl.BlockSpec(memory_space=pltpu.VMEM)
NT = 4
CB = 512
RING, LAG = 4, 2
LANES = 128
BLOCK = 512
VMEM_LIMIT = 63 * 2**20

OWN, PART, MATE, FAR = SLOTS = range(4)
S, T, F = KINDS = range(3)
KIND_OF = {MATE: S, PART: T, FAR: F}
GATE, UP = GU = range(2)
MINE, THEIRS = SEQS = range(2)


def scope(name):
    return jax.named_scope(name)


def timed(name):
    def wrap(f):
        @functools.wraps(f)
        def g(*args):
            with scope("_".join([name, *(str(a) for a in args if isinstance(a, int))])):
                return f(*args)
        return g
    return wrap


def dot(a, b):
    return jnp.dot(a, b, preferred_element_type=F32)


def remote(src, dst, s, q, dev):
    return pltpu.make_async_remote_copy(src_ref=src, dst_ref=dst, send_sem=s, recv_sem=q, device_id=dev, device_id_type=MESH)


local = pltpu.make_async_copy


def span(i, n):
    return pl.ds(pl.multiple_of(i * n, n), n)


def each(lo, hi):
    return pl.loop(lo, hi)


class Place:
    def __init__(self, chips, layer):
        self.chips = chips
        self.r = lax.axis_index('dp')
        self.j = lax.axis_index('mp')
        self.chip, self.core = self.j // 2, self.j % 2
        sides = 3 - self.r, self.r + 1 - 2 * (self.r % 2)
        odd = layer % 2
        self.slots = (self.r, sides[odd], sides[1 - odd], lax.rem(self.r + 2, 4))
        self.half = lax.rem((self.r + odd) // 2, 2)
        self.named = (OWN, MATE, PART, FAR) if odd else SLOTS
        self.partner, self.mate, self.across = ({'dp': s} for s in self.slots[1:])
        self.sib = {'mp': self.chip * 2 + 1 - self.core}
        self.next, self.prev = self.at(1), self.at(chips - 1)

    def chip_at(self, off):
        return lax.rem(self.chip + off, self.chips)

    def at(self, off):
        return {'mp': self.chip_at(off) * 2 + self.core}

    def meet(self, *peers):
        barrier = pltpu.get_barrier_semaphore()
        for p in peers:
            pl.semaphore_signal(barrier, inc=1, device_id=p, device_id_type=MESH)
        pl.semaphore_wait(barrier, len(peers))


class Pieces:
    def __init__(self, layer, wq, wg, wu, me):
        self.layer, self.me = layer, me
        self.wq, self.w = wq, (wg, wu)
        self.nq = wq.shape[2] // 2
        self.nf = wg.shape[2] // 2
        self.tile = self.nf // NT

    def q(self, half):
        return self.wq.at[self.layer, :, span(half, self.nq)]

    def g(self, half, which, t):
        return self.w[which].at[self.layer, :, span(half * NT + t, self.tile)]

    def tile_part(self, buf, which):
        return buf.at[:, pl.ds(which * self.tile, self.tile)]


def out_rows(layer, half, wo, wd):
    return [w.at[layer, span(half, w.shape[1] // 2), :] for w in (wo, wd)]


def split_rows(o, n):
    return [o.at[pl.ds(0, n), :]] + ([o.at[pl.ds(n, o.shape[0] - n), :]] if n < o.shape[0] else [])


def front_kernel(layer, chips, *refs):
    first = layer == 0
    it = iter(refs)
    take = lambda n: [next(it) for _ in range(n)]
    x, gam, lens, wq, wkv, wg, wu, wo, wd = take(9)
    if first:
        om, hbuf, s_o, t_o, sg1, wkvb, gb, lenb = take(8)
    else:
        sg1, wkvb, *ahead = take(8)
        om, hbuf, s_o, t_o = take(4)
        gb, lenb = gam, lens
    (wqkv, wgu, hv, qkv, hown, hpar, wkvp, sc, ms, os, y_s, y_r, ld, o_s, o_r, kv_sem, hv_sem, ms_sem, os_sem, ag_s, ag_r, own_sem,
     ex_s, ex_r) = it
    me = Place(chips, layer)
    pc = Pieces(layer, wq, wg, wu, me)
    mp = 2 * chips
    tok, d4, nq = x.shape[0], wq.shape[1], pc.nq
    dh = nq

    def at_slot(s, which, t):
        if which < GATE:
            return wqkv.at[s, :, pl.ds(0, nq)]
        return pc.tile_part(wgu.at[s, t], which)

    def raw(half, which, t):
        return pc.q(half) if which < GATE else pc.g(half, which, t)

    def given(kind, which, t):
        q, g = ahead[2 * kind:2 * kind + 2]
        if which < GATE:
            return q
        return pc.tile_part(sg1 if kind == S and t == EARLY else g.at[t], which)

    def sem(which, t):
        return 0 if which < GATE else 1 + 2 * t + which

    def load(s, which, t):
        src = raw(me.half, which, t) if s == OWN else given(KIND_OF[s], which, t)
        return local(src, at_slot(s, which, t), ld.at[s, sem(which, t)])

    def came(kind, t):
        return not first and (t is None or (isinstance(t, int) and (t < AHEAD[kind] or (kind == S and t == EARLY))))

    def move(kind, which, t):
        n = sem(which, t)
        sems = (y_s.at[kind, n], y_r.at[kind, n])
        if kind == S:
            return remote(raw(me.half, which, t), at_slot(MATE, which, t), *sems, me.mate)
        if kind == T:
            return remote(raw(1 - me.half, which, t), at_slot(PART, which, t), *sems, me.partner)
        src = given(T, which, t) if came(T, None if which < GATE else t) else at_slot(PART, which, t)
        return remote(src, at_slot(FAR, which, t), *sems, me.mate)

    def parts(t):
        return [(GATE - 1, 0)] if t is None else [(w, t) for w in GU]

    def send(kind, *ts):
        for t in ts:
            for p in parts(t):
                move(kind, *p).start()

    @timed('relay')
    def relay(*ts):
        for t in ts:
            for p in parts(t):
                if not came(T, t):
                    move(T, *p).wait_recv()
                move(F, *p).start()

    @timed('have')
    def have(*ts):
        for t in ts:
            for p in parts(t):
                load(OWN, *p).wait()
                if came(S, t):
                    load(MATE, *p).wait()
                else:
                    move(S, *p).wait_recv()
                if came(T, t):
                    load(PART, *p).wait()
                if came(F, t):
                    load(FAR, *p).wait()
                else:
                    move(F, *p).wait_recv()

    every = [None, *range(NT)]
    for t in every:
        for p in parts(t):
            load(OWN, *p).start()
            for s, kind in KIND_OF.items():
                if came(kind, t):
                    load(s, *p).start()

    with scope('meet'):
        me.meet(me.sib, me.next, me.prev, me.mate, me.partner, *([me.across] if first else []))

    own_o, oth_o = out_rows(layer, me.half, wo, wd), out_rows(layer, 1 - me.half, wo, wd)
    no = wo.shape[1] // 2
    ahead_o = zip(oth_o + [own_o[0], own_o[1].at[pl.ds(0, s_o.shape[0] - no), :]], split_rows(t_o, no) + split_rows(s_o, no),
                  [me.partner, me.partner, me.mate, me.mate])
    out_moves = [remote(src, dst, o_s.at[n], o_r.at[n], dev) for n, (src, dst, dev) in enumerate(ahead_o)]

    if first:
        then = Place(chips, layer + 1)
        pn = Pieces(layer + 1, wq, wg, wu, then)
        out_moves += [remote(pn.g(then.half, which, EARLY), pc.tile_part(sg1, which), o_s.at[4 + which], o_r.at[4 + which], then.mate) for which in GU]

    small = []
    if first:
        kv_own = local(wkv.at[:, span(me.j, wkv.shape[1] // mp), :], wkvp.at[:, OWN], own_sem.at[4])
        kv_own.start()
        for s, dev in ((PART, me.partner), (MATE, me.mate), (FAR, me.across)):
            small.append(remote(gam, gb.at[s], ex_s.at[s], ex_r.at[s], dev))
        for s, dev in ((PART, me.partner), (MATE, me.mate)):
            small.append(remote(lens, lenb.at[s], ex_s.at[7 + s], ex_r.at[7 + s], dev))
        for c in small:
            c.start()
        gb[OWN] = gam[:, :]
        lenb[OWN] = lens[:, :]
        kv_own.wait()

        def kv_move(kind):
            src, dst, dev = ((OWN, MATE, me.mate), (OWN, PART, me.partner), (PART, FAR, me.mate))[kind]
            return remote(wkvp.at[:, src], wkvp.at[:, dst], ex_s.at[4 + kind], ex_r.at[4 + kind], dev)
        for k in (T, S):
            kv_move(k).start()
            send(k, 0)
        with scope('small'):
            for c in small:
                c.wait_recv()
    else:
        relay(1)
        send(S, 2, 3)

    @timed('norm')
    def norm():
        rb = 32

        @each(0, tok // rb)
        def _(i):
            rows = span(i, rb)
            xf = x[rows, :].astype(F32)
            mu = jnp.mean(xf, axis=-1, keepdims=True)
            xc = xf - mu
            rstd = lax.rsqrt(jnp.mean(xc * xc, axis=-1, keepdims=True) + EPS)
            for s in SLOTS:
                cols = span(me.slots[s], d4)
                hown[rows, cols] = ((x[rows, cols].astype(F32) - mu) * rstd * gb[me.named[s], layer:layer + 1, :]).astype(BF)
    norm()

    SIB, TO, SHARE, PASS, LAST = range(5)

    def gather(g, src, block, part):
        offs = (chips - 1, 1)
        dirs = (me.next, me.prev)

        def idx(off):
            return me.chip_at(off) * 2 + me.core

        def c(kind, k, h):
            n = 4 * kind + 2 * k + h
            sems = (ag_s.at[g, n], ag_r.at[g, n])
            if kind == SIB:
                return remote(src, block(me.j), *sems, me.sib)
            if kind == TO:
                return remote(part(src, h), part(block(me.j), h), *sems, dirs[k])
            b = part(block(idx(2 if kind == LAST else offs[k])), h)
            return remote(b, b, *sems, dirs[k] if kind == PASS else me.sib)

        mine = local(src, block(me.j), own_sem.at[g])
        tag = 'abvw'[g]

        class G:
            @timed('own' + tag)
            def own():
                for h in range(2):
                    for k in range(2):
                        c(TO, k, k ^ h).start()
                c(SIB, 0, 0).start()
                mine.start()

            @timed('near' + tag)
            def near():
                for h in range(2):
                    for k in range(2):
                        c(TO, k, k ^ h).wait_recv()
                        if h == 0:
                            c(PASS, k, k).start()
                        c(SHARE, k, k ^ h).start()

            @timed('far' + tag)
            def far():
                for k in range(2):
                    c(PASS, k, k).wait_recv()
                    c(LAST, k, k).start()

            @timed('has' + tag)
            def has(kind):
                if kind == SIB:
                    mine.wait()
                    c(SIB, 0, 0).wait_recv()
                for k in range(2):
                    if kind == LAST:
                        c(kind, k, k).wait_recv()
                    if kind == SHARE:
                        for h in range(2):
                            c(kind, k, k ^ h).wait_recv()

            def end():
                c(SIB, 0, 0).wait_send()
                for k in range(2):
                    for h in range(2):
                        c(TO, k, h).wait_send()
                        c(SHARE, k, h).wait_send()
                    c(PASS, k, k).wait_send()
                    c(LAST, k, k).wait_send()
        return G

    def h_block(b):
        return lambda j: hbuf.at[b, span(j, tok), :]

    def h_part(ref, k):
        return ref.at[pl.ds(k * (tok // 2), tok // 2), :]

    ga, gb2 = gather(0, hown, h_block(MINE), h_part), gather(1, hpar, h_block(THEIRS), h_part)
    ht = remote(hown, hpar, ex_s.at[7], ex_r.at[7], me.partner)

    rows2 = 2 * tok

    def chip_rows(i):
        return span(me.chip_at(i + i // 2 - 2 * (i // 3)), rows2)

    def hload(i):
        return local(hbuf.at[i // chips, chip_rows(lax.rem(i, chips)), :], hv.at[lax.rem(i, 2), pl.ds(0, rows2), :], hv_sem.at[lax.rem(i, 2)])

    def hdot(i, rows, w):
        acc = None
        for s in SLOTS:
            p = dot(hv[lax.rem(i, 2), :rows, span(me.slots[s], d4)], w(s))
            acc = p if acc is None else acc + p
        return acc

    def mcopy(b, rows, n, t, k):
        w = pc.tile
        return local(ms.at[k, pl.ds(0, n), :], om.at[b, rows, pl.ds(pl.multiple_of(nq + t * w, w), w)], ms_sem.at[k])

    def tile(i, b, rows, n, t, m):
        k = lax.rem(m, 2)
        a = hdot(i, n, lambda s: wgu[s, t])

        @pl.when(m >= 2)
        def _():
            mcopy(b, rows, n, t, k).wait()
        gt = a[:, :pc.tile].astype(BF).astype(F32)
        up = a[:, pc.tile:].astype(BF).astype(F32)
        ms[k, :n, :] = (gt * jax.nn.sigmoid(gt) * up).astype(BF)
        mcopy(b, rows, n, t, k).start()

    def drain(n):
        for k in range(2):
            mcopy(MINE, pl.ds(0, n), n, 0, k).wait()

    def any_of(i, marks):
        return functools.reduce(lambda a, b: a | b, [i == g for g in marks])

    def sweep(b, qk, nt, gates, hooks):
        lo = b * chips
        marks = [n for n in gates]

        @each(lo, lo + chips)
        def _(i):
            for g, f in gates.items():
                pl.when(i == g)(f)

            @pl.when(any_of(i, [lo, *marks]))
            def _():
                hload(i).start()

            @pl.when(jnp.logical_not(any_of(i + 1, [lo + chips, *marks])))
            def _():
                hload(i + 1).start()
            hload(i).wait()
            rows = chip_rows(i - lo)
            if qk:
                qkv[b, rows, :] = hdot(i, rows2, lambda s: wqkv[s]).astype(BF)

            @each(0, nt)
            def _(t):
                for n, f in hooks.items():
                    pl.when((i == lo) & (b == MINE) & (t == n))(f)
                tile(i, b, rows, rows2, t, (i - lo) * nt + t)

        @pl.when(nt + lo >= 1)
        def _():
            drain(rows2)

    def late(lo_t, hi_t, lo, hi, hooks):
        big = hv.shape[1]
        per = qkv.shape[1] // big
        n = (hi - lo) * per

        def place(u):
            v = lo * per + lax.rem(u, n)
            return v // per, span(lax.rem(v, per), big)

        def load_big(u):
            b, rows = place(u)
            return local(hbuf.at[b, rows, :], hv.at[lax.rem(u, 2)], hv_sem.at[lax.rem(u, 2)])

        def run():
          @each(0, n * (hi_t - lo_t))
          def _(u):
            t = lo_t if hi_t - lo_t == 1 else lo_t + u // n

            @pl.when(lax.rem(u, n) == 0)
            def _():
                have(t)
            for k, f in hooks.items():
                pl.when(u == k)(f)

            @pl.when(u + 1 < n * (hi_t - lo_t))
            def _():
                load_big(u + 1).start()
            load_big(u).wait()
            b, rows = place(u)
            tile(u, b, rows, big, t, u)
          drain(big)
        return load_big(0).start, run

    bq, bk = sc.shape[1:]

    @timed('attend')
    def attend(b):
        nblk = qkv.shape[1] // bq
        ratio = bk // bq

        def ocp(i, k):
            return local(os.at[k], om.at[b, span(i, bq), pl.ds(0, dh)], os_sem.at[k])

        def lanes(a, op):
            return functools.reduce(op, [a[:, n * LANES:(n + 1) * LANES] for n in range(bk // LANES)])

        @each(0, nblk)
        def _(i):
            q = qkv[b, span(i, bq), pl.ds(0, dh)]
            length = lenb[b * me.named[PART], :, :][:1, :1]
            colf = lax.broadcasted_iota(jnp.int32, (1, bk), 1).astype(F32)

            def raw_score(j):
                k = qkv[b, span(j, bk), pl.ds(dh, dh)]
                s = lax.dot_general(q, k, (((1,), (1,)), ((), ())), preferred_element_type=F32) * (dh ** -0.5)
                pos = jnp.broadcast_to(colf + (j * bk).astype(F32), (bq, bk))
                return jnp.where(pos < length, s, -1e30)

            def score(j, m):
                s = raw_score(j)
                sc[j] = s
                return jnp.maximum(m, lanes(s, jnp.maximum))

            last = i // ratio
            row = lax.broadcasted_iota(jnp.int32, (bq, bk), 0) + (i - last * ratio) * bq
            col = lax.broadcasted_iota(jnp.int32, (bq, bk), 1)
            s = jnp.where(col <= row, raw_score(last), -1e30)
            sc[last] = s
            m = jnp.max(lax.fori_loop(0, last, score, lanes(s, jnp.maximum)), axis=1, keepdims=True)

            def expo(j, l):
                p = jnp.exp(sc[j] - m)
                sc[j] = p
                return l + lanes(p, jnp.add)

            l = jnp.sum(lax.fori_loop(0, last + 1, expo, jnp.zeros((bq, LANES), F32)), axis=1, keepdims=True)
            inv = 1.0 / l

            def value(j, o):
                return o + dot((sc[j] * inv).astype(BF), qkv[b, span(j, bk), pl.ds(2 * dh, dh)])

            o = lax.fori_loop(0, last + 1, value, jnp.zeros((bq, dh), F32))
            k = lax.rem(i, 2)

            @pl.when(i >= 2)
            def _():
                ocp(i, k).wait()
            os[k] = o.astype(BF)
            ocp(i, k).start()
        for k in range(2):
            ocp(k, k).wait()

    def kv_load(u):
        s, j = u // mp, lax.rem(u, mp)
        name = s if first else s + (1 - s // 3) * (s - s // 2 * 2 - s // 2 * 1)
        return local(wkvb.at[layer, j, s], wqkv.at[name, span(j, wkvp.shape[2]), pl.ds(nq, 2 * dh)], kv_sem.at[u])

    def kv_loads(go):
        @each(0, 4 * mp)
        def _(u):
            go(kv_load(u))

    def near_of(g):
        def f():
            g.near()
            g.has(SHARE)
        return f

    def far_of(g):
        def f():
            g.far()
            g.has(LAST)
        return f

    def both(*fs):
        def f():
            for g in fs:
                g()
        return f

    def start_b():
        with scope('ht'):
            ht.wait_recv()
        gb2.own()

    ga.own()
    if first:
        with scope('kvmove'):
            kv_move(T).wait_recv()
            kv_move(F).start()
        send(T, None)
        with scope('kvmove2'):
            kv_move(S).wait_recv()
            kv_move(F).wait_recv()
        gw = [gather(2 + n, wkvp.at[n], lambda j, n=n: wkvb.at[n, j], lambda ref, k: ref.at[pl.ds(2 * k, 2)]) for n in range(2)]
        relay(0)
        send(S, None)
        ht.start()
        relay(None)
        ga.near()
        gw[0].own()
        for kind in (SIB, SHARE):
            ga.has(kind)
        have(0)
        send(S, 1)
        send(T, 1)
        send(S, 2)

        def far_a():
            ga.far()
            ga.has(LAST)
        with scope('pre'):
            sweep(MINE, False, 1, {3: far_a}, {})
        gw[0].near()
        start_b()
        send(T, 2)
        send(T, 3)
        gw[0].far()
        for c in out_moves[:2]:
            c.start()
        for kind in (SIB, SHARE, LAST):
            gw[0].has(kind)
        kv_loads(lambda c: c.start())
        kv_loads(lambda c: c.wait())
        have(None)
        load_late, run_late = late(1, NT, MINE, len(SEQS), {4: gw[1].near, 8: gw[1].far})

        @each(0, 2)
        def _(b):
            with scope('sweep'):
                sweep(b, True, b, {chips: lambda: gb2.has(SIB), chips + 1: both(near_of(gb2), lambda: relay(2)),
                                   chips + 3: far_of(gb2)}, {})

            @pl.when(b == MINE)
            def _():
                relay(1)
                send(S, 3)

            @pl.when(b == THEIRS)
            def _():
                relay(3)
                for c in out_moves[2:]:
                    c.start()
                gw[1].own()
                load_late()
            attend(b)

        with scope('late'):
            run_late()
        for kind in (SIB, SHARE, LAST):
            gw[1].has(kind)
    else:
        ht.start()
        send(T, 2, 3)
        for c in out_moves[:2]:
            c.start()
        kv_loads(lambda c: c.start())
        kv_loads(lambda c: c.wait())
        have(None, 0)

        def far_a():
            far_of(ga)()
            relay(2)
        load_some, run_some = late(2, 3, MINE, THEIRS, {})
        load_late, run_late = late(3, NT, MINE, len(SEQS), {})

        @each(0, 2)
        def _(b):
            with scope('sweep'):
                sweep(b, True, 2 + b, {0: lambda: ga.has(SIB), 1: both(near_of(ga), start_b), 3: far_a,
                                       chips: both(lambda: gb2.has(SIB), gb2.near), chips + 1: lambda: gb2.has(SHARE), chips + 3: far_of(gb2)},
                      {1: lambda: have(1)})
            pl.when(b == MINE)(load_some)
            pl.when(b == THEIRS)(load_late)
            attend(b)

            @pl.when(b == MINE)
            def _():
                relay(3)
                for c in out_moves[2:]:
                    c.start()
                with scope('late2'):
                    run_some()
        with scope('late'):
            run_late()

    with scope('end'):
        for t in every:
            for p in parts(t):
                for k in KINDS:
                    if not came(k, t):
                        move(k, *p).wait_send()
        for c in out_moves:
            c.wait()
        ht.wait_send()
        ga.end()
        gb2.end()
        for c in small:
            c.wait_send()
        if first:
            gw[0].end()
            gw[1].end()
            for k in KINDS:
                kv_move(k).wait_send()


EARLY = 1
AHEAD = (1, 2, 1)


def front(layer, mesh, x, gam, lens, weights, given):
    wq, wkv, wg, wu, wo, wd = weights
    tok, d = x.shape
    mp = mesh.shape['mp']
    chips = mp // 2
    first = layer == 0
    d4 = wq.shape[1]
    nq, nkv, nf = wq.shape[2] // 2, wkv.shape[2], wg.shape[2] // 2
    no, nd = wo.shape[1] // 2, wd.shape[1] // 2
    t = tok * mp
    kvr = wkv.shape[1] // mp
    sds = jax.ShapeDtypeStruct
    outs = [sds((2, t, nq + nf), BF), sds((2, t, d), BF), sds((no + (nd // 2 if first else nd), d4), BF), sds((no + nd, d4), BF)]
    specs = [ANY] * 4
    if first:
        outs += [sds((d4, 2 * nf // NT), BF), sds((2, mp, 4, kvr, nkv), BF), sds((4, *gam.shape), F32), sds((3, *lens.shape), F32)]
        specs += [ANY, ANY, VM, VM]
    npiece = 1 + 2 * NT
    return pl.pallas_call(
        functools.partial(front_kernel, layer, chips), out_shape=outs,
        in_specs=[VM, VM, VM] + [ANY] * (6 + len(given)), out_specs=specs,
        scratch_shapes=[
            pltpu.VMEM((4, d4, nq + nkv), BF), pltpu.VMEM((4, NT, d4, 2 * nf // NT), BF), pltpu.VMEM((2, 4 * tok, d), BF),
            pltpu.VMEM((2, t, nq + nkv), BF), pltpu.VMEM((tok, d), BF), pltpu.VMEM((tok, d), BF),
            pltpu.VMEM((2, 4, kvr, nkv), BF), pltpu.VMEM((t // BLOCK, BLOCK, BLOCK), F32),
            pltpu.VMEM((2, 4 * tok, nf // NT), BF), pltpu.VMEM((2, BLOCK, nq), BF),
            DMA((3, npiece)), DMA((3, npiece)), DMA((4, npiece)), DMA((6,)), DMA((6,)), DMA((4 * mp,)), DMA((2,)), DMA((2,)), DMA((2,)),
            DMA((4, 20)), DMA((4, 20)), DMA((5,)), DMA((10,)), DMA((10,))],
        compiler_params=pltpu.CompilerParams(vmem_limit_bytes=VMEM_LIMIT, collective_id=2 * layer, has_side_effects=True),
        cost_estimate=pl.CostEstimate(flops=4 * t * d * (nq + nkv + 2 * nf), bytes_accessed=12 * t * d, transcendentals=0),
        name=f"front{layer}")(x, gam, lens, *weights, *given)


def back_kernel(layer, chips, nxt, *refs):
    it = iter(refs)
    take = lambda n: [next(it) for _ in range(n)]
    x, om_h, s_o, t_o, wo, wd = take(6)
    if nxt:
        wq, wg, wu = take(3)
    y = next(it)
    if nxt:
        bufs = take(6)
    (om, w, sl, rel, fin, zt, sib, acc, in_sem, w_s, w_r, p_s, p_r, sib_s, sib_r, rel_s, rel_r, fin_s, fin_r, t_s, t_r) = it
    me = Place(chips, layer)
    nb, rows = zt.shape[:2]
    per = w.shape[2] // CB
    no, ns = wo.shape[1] // 2, s_o.shape[0]

    own_o = out_rows(layer, me.half, wo, wd)
    own_rows, mate_rows = split_rows(w.at[OWN], no), split_rows(w.at[MATE], ns)
    loads = [local(om_h.at[THEIRS], om.at[THEIRS], in_sem.at[0]), local(own_o[0], own_rows[0], in_sem.at[1]),
             local(own_o[1], own_rows[1], in_sem.at[2]), local(t_o, w.at[PART], in_sem.at[3]), local(om_h.at[MINE], om.at[MINE], in_sem.at[4]),
             local(s_o, mate_rows[0], in_sem.at[5])]
    for c in loads[:3]:
        c.start()
    me.meet(me.sib, me.next, me.prev, me.mate, me.partner)
    for c in loads[3:]:
        c.start()
    to_mate = [remote(t_o.at[:, span(n, CB)], w.at[FAR, :, span(n, CB)], w_s.at[n], w_r.at[n], me.mate) for n in range(per)]
    if nxt:
        to_mate.insert(0, remote(own_o[1].at[pl.ds(ns - no, no + own_o[1].shape[0] - ns), :], mate_rows[1], w_s.at[per], w_r.at[per], me.mate))
    else:
        for c in to_mate:
            c.start()
    passing = []
    if nxt:
        then = Place(chips, layer + 1)
        pc = Pieces(layer + 1, wq, wg, wu, then)

        def ahead(kind, dev):
            q, g = bufs[2 * kind:2 * kind + 2]
            dst = [q] + [pc.tile_part(g.at[t], which) for t in range(AHEAD[kind]) for which in GU]
            if kind == F:
                q, g = bufs[2 * T:2 * T + 2]
                src = [q] + [pc.tile_part(g.at[t], which) for t in range(AHEAD[F]) for which in GU]
            else:
                half = then.half if kind == S else 1 - then.half
                src = [pc.q(half)] + [pc.g(half, which, t) for t in range(AHEAD[kind]) for which in GU]
            return [remote(*sd, p_s.at[kind, n], p_r.at[kind, n], dev) for n, sd in enumerate(zip(src, dst))]
        to_s, to_t, on = ahead(S, then.mate), ahead(T, then.partner), ahead(F, then.mate)
        for c in (*to_t[:len(on)], *to_mate, *to_s, *to_t[len(on):]):
            c.start()
        passing = to_s + on + to_t[len(on):]
    with scope('loads'):
        for c in loads[:4]:
            c.wait()

    AWAY, NEAR, JOIN, HOME = range(4)

    def sib_copy(st, b, cb, m):
        k = lax.rem(m, RING)
        return remote(sib.at[k], sl.at[st, b, cb], sib_s.at[k], sib_r.at[st, b, cb], me.sib)

    def away_copy(b, cb):
        return remote(sl.at[AWAY, b, cb], rel.at[b, cb], rel_s.at[b, cb], rel_r.at[b, cb], me.at(1 + 2 * lax.rem(cb, 2)))

    def near_copy(st, b, cb):
        p = lax.rem(st + cb, 2)
        return remote(sl.at[st, b, cb], fin.at[p, b, cb], fin_s.at[p, b, cb], fin_r.at[p, b, cb], me.at(1 + 2 * p))

    def compute(off, st, b, cb, m):
        a = acc.at[lax.rem(m, LAG + 1)]
        a[:, :] = dot(om[b, span(me.chip_at(off), 2 * rows), :], w[cb // per, :, span(lax.rem(cb, per), CB)])

        @pl.when(m >= RING)
        def _():
            sib_copy(st, b, cb, m).wait_send()
        sib[lax.rem(m, RING)] = a[span(1 - me.core, rows), :].astype(BF)
        sib_copy(st, b, cb, m).start()

    def combined(st, b, cb, m):
        sib_copy(st, b, cb, m).wait_recv()
        a = acc.at[lax.rem(m, LAG + 1)]
        return a[span(me.core, rows), :] + sl[st, b, cb].astype(F32)

    def run(n, unit, off, finish):
        @each(0, n + LAG)
        def _(m):
            @pl.when(m < n)
            def _():
                st, b, cb = unit(m)
                compute(off(st, cb), st, b, cb, m)

            @pl.when(m >= LAG)
            def _():
                st, b, cb = unit(m - LAG)
                finish(st, b, cb, combined(st, b, cb, m - LAG))

        for m in range(RING):
            @pl.when(m < n)
            def _(m=m):
                sib_copy(HOME, MINE, 0, m).wait_send()

    @timed('depart')
    def depart(lo, n):
        def unit(m):
            return m // (2 * n), 1 - lax.rem(m // n, 2), lo + lax.rem(m, n)

        def off(st, cb):
            return (1 - st) * 2 + st * (1 + 2 * lax.rem(st + cb, 2))

        def on(st, b, cb, v):
            sl[st, b, cb] = v.astype(BF)

            @pl.when(st == AWAY)
            def _():
                away_copy(b, cb).start()

            @pl.when(st == NEAR)
            def _():
                near_copy(NEAR, b, cb).start()
        run(4 * n, unit, off, on)

    @timed('join')
    def join(lo, n):
        def unit(m):
            return JOIN + m // (2 * n), 1 - lax.rem(m // n, 2), lo + lax.rem(m, n)

        def off(st, cb):
            return (HOME - st) * (1 + 2 * lax.rem(st + cb, 2))

        def on(st, b, cb, v):
            @pl.when(st == JOIN)
            def _():
                away_copy(b, cb).wait_recv()
                sl[JOIN, b, cb] = (v + rel[b, cb].astype(F32)).astype(BF)
                near_copy(JOIN, b, cb).start()

            @pl.when(st == HOME)
            def _():
                sl[HOME, b, cb] = v.astype(BF)
        run(4 * n, unit, off, on)

    def t_copy(cb):
        return remote(sl.at[HOME, THEIRS, cb], zt.at[cb], t_s.at[cb], t_r.at[cb], me.partner)

    def total(b, cb):
        for p in range(2):
            local(fin.at[p, b, cb], fin.at[p, b, cb], fin_r.at[p, b, cb]).wait()
        return sl[HOME, b, cb].astype(F32) + fin[0, b, cb].astype(F32) + fin[1, b, cb].astype(F32)

    @timed('theirs')
    def theirs(lo, hi):
        @each(lo, hi)
        def _(cb):
            sl[HOME, THEIRS, cb] = total(THEIRS, cb).astype(BF)
            t_copy(cb).start()

    def swapped(cb):
        slot = cb // per
        return (slot + 1 - 2 * (slot % 2)) * per + cb % per

    def give_copy(st, cb):
        if st == HOME:
            return t_copy(cb)
        if st == AWAY:
            dst, *sems = rel.at[THEIRS, cb], rel_s.at[THEIRS, cb], rel_r.at[THEIRS, cb]
        else:
            p = st - NEAR
            dst, *sems = fin.at[p, THEIRS, cb], fin_s.at[p, THEIRS, cb], fin_r.at[p, THEIRS, cb]
        return remote(sl.at[st, THEIRS, cb], dst, *sems, me.partner)

    def given(st, cb):
        c = swapped(cb)
        give_copy(st, c).wait_recv()
        return (rel[THEIRS, c] if st == AWAY else zt[c] if st == HOME else fin[st - NEAR, THEIRS, c]).astype(F32)

    def offset(st, cb):
        first, home = (HOME - st) // HOME, st // HOME
        return 2 * first + (1 - first) * (1 - home) * (1 + 2 * lax.rem(st + cb, 2))

    @timed('give')
    def give(lo, n):
        def unit(m):
            return lax.rem(m, 4), THEIRS, swapped(lo + m // 4)

        def on(st, b, cb, v):
            sl[st, THEIRS, cb] = v.astype(BF)
            for k in (AWAY, NEAR, JOIN, HOME):
                @pl.when(st == k)
                def _(k=k):
                    give_copy(k, cb).start()
        run(4 * n, unit, offset, on)

    @timed('take')
    def take(lo, n):
        def unit(m):
            k = lax.rem(m, 4)
            return k + k // 2 - 2 * (k // 3), MINE, lo + m // 4

        def on(st, b, cb, v):
            for k in (AWAY, NEAR, JOIN, HOME):
                @pl.when(st == k)
                def _(k=k):
                    z = v + given(k, cb)
                    if k == JOIN:
                        away_copy(MINE, cb).wait_recv()
                        z = z + rel[MINE, cb].astype(F32)
                    sl[k, MINE, cb] = z.astype(BF)
                    if k == AWAY:
                        away_copy(MINE, cb).start()
                    elif k != HOME:
                        near_copy(k, MINE, cb).start()
        run(4 * n, unit, offset, on)

    @timed('mine')
    def mine(slot, with_theirs):
        @each(0, per)
        def _(n):
            cb = slot * per + n
            z = total(MINE, cb)
            if with_theirs:
                t_copy(swapped(cb)).wait_recv()
                z = z.astype(BF).astype(F32) + zt[swapped(cb)].astype(F32)
            cols = span(me.slots[slot] * per + n, CB)
            y[:, cols] = (x[:, cols].astype(F32) + z).astype(BF)

    def wait_rest():
        loads[4].wait()
        loads[5].wait()

    if nxt:
        @each(0, 4)
        def _(g):
            n = 2 * per // (1 + g)
            lo = nb - 2 * n + g // 3
            pl.when(g == 0)(wait_rest)
            for k in range(len(to_mate)):
                @pl.when(g == 1 + k)
                def _(k=k):
                    with scope('w%d' % k):
                        to_mate[k].wait_recv()
            depart(lo, n)

            @pl.when(g == 0)
            def _():
                join(lo, n)
                with scope('passing'):
                    for t, f in zip(to_t, on):
                        t.wait_recv()
                        f.start()

            @pl.when(g == 1)
            def _():
                theirs(0, 2 * per)

            @pl.when(g == 2)
            def _():
                join(2 * per, per)
                theirs(2 * per, 3 * per)
        join(3 * per, per)
        theirs(3 * per, nb)
    else:
        @each(0, 2)
        def _(g):
            give(g, 1 + 2 * g)

            @pl.when(g == 0)
            def _():
                wait_rest()

            @pl.when(g == 1)
            def _():
                take(per * OWN, per)
                theirs(per * MATE, per * FAR)
                with scope('w'):
                    for c in to_mate:
                        c.wait_recv()
            depart(per * (MATE + g), per)
            join(per * (MATE + g), per)
        take(per * PART, per)
        theirs(per * FAR, nb)
    for slot in SLOTS:
        mine(slot, nxt or slot in (MATE, FAR))

    with scope('end'):
        @each(0, nb)
        def _(cb):
            t_copy(cb).wait_send()
            for b in SEQS:
                away_copy(b, cb).wait_send()
                for st in (NEAR, JOIN):
                    near_copy(st, b, cb).wait_send()
        for c in to_mate:
            c.wait_send()
        for c in passing:
            c.wait()
        if nxt:
            for c in to_t[:len(on)]:
                c.wait_send()


def back(layer, mesh, x, om, s_o, t_o, weights, last):
    wq, wkv, wg, wu, wo, wd = weights
    mp = mesh.shape['mp']
    tok, d = x.shape
    t, k = om.shape[1:]
    d4 = wo.shape[2]
    nb = d // CB
    unit = (tok, CB)
    nq, nf = wq.shape[2] // 2, wg.shape[2] // 2
    sds = jax.ShapeDtypeStruct
    outs, specs = [sds((tok, d), BF)], [VM]
    args = [x, om, s_o, t_o, wo, wd]
    if not last:
        args += [wq, wg, wu]
        for n in AHEAD:
            outs += [sds((d4, nq), BF), sds((n, d4, 2 * nf // NT), BF)]
        specs += [ANY] * 6
    npiece = 1 + 2 * NT
    return pl.pallas_call(
        functools.partial(back_kernel, layer, mp // 2, not last), out_shape=outs,
        in_specs=[VM] + [ANY] * (len(args) - 1), out_specs=specs,
        scratch_shapes=[
            pltpu.VMEM((2, t, k), BF), pltpu.VMEM((4, k, d4), BF),
            pltpu.VMEM((4, 2, nb, *unit), BF), pltpu.VMEM((2, nb, *unit), BF), pltpu.VMEM((2, 2, nb, *unit), BF), pltpu.VMEM((nb, *unit), BF),
            pltpu.VMEM((RING, *unit), BF), pltpu.VMEM((LAG + 1, 2 * tok, CB), F32),
            DMA((6,)), DMA((3,)), DMA((3,)), DMA((3, npiece)), DMA((3, npiece)), DMA((RING,)), DMA((4, 2, nb)),
            DMA((2, nb)), DMA((2, nb)), DMA((2, 2, nb)), DMA((2, 2, nb)), DMA((nb,)), DMA((nb,))],
        compiler_params=pltpu.CompilerParams(vmem_limit_bytes=VMEM_LIMIT, collective_id=2 * layer + 1, has_side_effects=True),
        cost_estimate=pl.CostEstimate(flops=4 * t * k * d, bytes_accessed=2 * (2 * t * k + 4 * k * d4), transcendentals=0),
        name=f"back{layer}")(*args)


def solution(mesh):
    assert mesh.shape['dp'] == len(SLOTS)

    def body(x, lengths, gamma, *weights):
        layers = gamma.shape[0]
        assert layers == 2
        x = x[0]
        gam = jnp.zeros((8, gamma.shape[1]), F32).at[:layers].set(gamma.astype(F32))
        lens = jnp.broadcast_to(lengths.astype(F32)[:, None], (8, 128))
        om, _, s_o, t_o, sg1, wkvb, gam, lens = front(0, mesh, x, gam, lens, weights, ())
        x, *ahead = back(0, mesh, x, om, s_o, t_o, weights, False)
        om, _, s_o, t_o = front(1, mesh, x, gam, lens, weights, (sg1, wkvb, *ahead))
        (x,) = back(1, mesh, x, om, s_o, t_o, weights, True)
        return x[None]

    in_specs = (P(('rep', 'dp'), 'mp', None), P(('rep', 'dp')), P(None, 'dp'),
                P(None, 'dp', 'mp'), P(None, 'dp', None), P(None, 'dp', 'mp'),
                P(None, 'dp', 'mp'), P(None, 'mp', 'dp'), P(None, 'mp', 'dp'))
    return jax.shard_map(body, mesh=mesh, in_specs=in_specs,
                         out_specs=P(('rep', 'dp'), 'mp', None), check_vma=False)
```

```python
import functools
import jax
import jax.numpy as jnp
from jax import lax
from jax.experimental import pallas as pl
from jax.experimental.pallas import tpu as pltpu
from jax.sharding import PartitionSpec as P

EPS = 1e-6
BF = jnp.bfloat16
F32 = jnp.float32
MESH = pl.DeviceIdType.MESH
DMA = pltpu.SemaphoreType.DMA
ANY = pl.BlockSpec(memory_space=pl.ANY)
VM = pl.BlockSpec(memory_space=pltpu.VMEM)
NT = 4
CB = 512
RING, LAG = 4, 2
LANES = 128
BLOCK = 512
VMEM_LIMIT = 63 * 2**20

OWN, PART, MATE, FAR = SLOTS = range(4)
S, T, F = KINDS = range(3)
KIND_OF = {MATE: S, PART: T, FAR: F}
GATE, UP = GU = range(2)
MINE, THEIRS = SEQS = range(2)


def scope(name):
    return jax.named_scope(name)


def timed(name):
    def wrap(f):
        @functools.wraps(f)
        def g(*args):
            with scope("_".join([name, *(str(a) for a in args if isinstance(a, int))])):
                return f(*args)
        return g
    return wrap


def dot(a, b):
    return jnp.dot(a, b, preferred_element_type=F32)


def remote(src, dst, s, q, dev):
    return pltpu.make_async_remote_copy(src_ref=src, dst_ref=dst, send_sem=s, recv_sem=q, device_id=dev, device_id_type=MESH)


local = pltpu.make_async_copy


def span(i, n):
    return pl.ds(pl.multiple_of(i * n, n), n)


def each(lo, hi):
    return pl.loop(lo, hi)


class Place:
    def __init__(self, chips, layer):
        self.chips = chips
        self.r = lax.axis_index('dp')
        self.j = lax.axis_index('mp')
        self.chip, self.core = self.j // 2, self.j % 2
        sides = 3 - self.r, self.r + 1 - 2 * (self.r % 2)
        odd = layer % 2
        self.slots = (self.r, sides[odd], sides[1 - odd], lax.rem(self.r + 2, 4))
        self.half = lax.rem((self.r + odd) // 2, 2)
        self.named = (OWN, MATE, PART, FAR) if odd else SLOTS
        self.partner, self.mate, self.across = ({'dp': s} for s in self.slots[1:])
        self.sib = {'mp': self.chip * 2 + 1 - self.core}
        self.next, self.prev = self.at(1), self.at(chips - 1)

    def chip_at(self, off):
        return lax.rem(self.chip + off, self.chips)

    def at(self, off):
        return {'mp': self.chip_at(off) * 2 + self.core}

    def meet(self, *peers):
        barrier = pltpu.get_barrier_semaphore()
        for p in peers:
            pl.semaphore_signal(barrier, inc=1, device_id=p, device_id_type=MESH)
        pl.semaphore_wait(barrier, len(peers))


class Pieces:
    def __init__(self, layer, wq, wg, wu, me):
        self.layer, self.me = layer, me
        self.wq, self.w = wq, (wg, wu)
        self.nq = wq.shape[2] // 2
        self.nf = wg.shape[2] // 2
        self.tile = self.nf // NT

    def q(self, half):
        return self.wq.at[self.layer, :, span(half, self.nq)]

    def g(self, half, which, t):
        return self.w[which].at[self.layer, :, span(half * NT + t, self.tile)]

    def tile_part(self, buf, which):
        return buf.at[:, pl.ds(which * self.tile, self.tile)]


def out_rows(layer, half, wo, wd):
    return [w.at[layer, span(half, w.shape[1] // 2), :] for w in (wo, wd)]


def split_rows(o, n):
    return [o.at[pl.ds(0, n), :]] + ([o.at[pl.ds(n, o.shape[0] - n), :]] if n < o.shape[0] else [])


def front_kernel(layer, chips, *refs):
    first = layer == 0
    it = iter(refs)
    take = lambda n: [next(it) for _ in range(n)]
    x, gam, lens, wq, wkv, wg, wu, wo, wd = take(9)
    if first:
        om, hbuf, s_o, t_o, sg1, wkvb, gb, lenb = take(8)
    else:
        sg1, wkvb, *ahead = take(8)
        om, hbuf, s_o, t_o = take(4)
        gb, lenb = gam, lens
    (wqkv, wgu, hv, qkv, hown, hpar, wkvp, sc, ms, os, y_s, y_r, ld, o_s, o_r, kv_sem, hv_sem, ms_sem, os_sem, ag_s, ag_r, own_sem,
     ex_s, ex_r) = it
    me = Place(chips, layer)
    pc = Pieces(layer, wq, wg, wu, me)
    mp = 2 * chips
    tok, d4, nq = x.shape[0], wq.shape[1], pc.nq
    dh = nq

    def at_slot(s, which, t):
        if which < GATE:
            return wqkv.at[s, :, pl.ds(0, nq)]
        return pc.tile_part(wgu.at[s, t], which)

    def raw(half, which, t):
        return pc.q(half) if which < GATE else pc.g(half, which, t)

    def given(kind, which, t):
        q, g = ahead[2 * kind:2 * kind + 2]
        if which < GATE:
            return q
        return pc.tile_part(sg1 if kind == S and t == EARLY else g.at[t], which)

    def sem(which, t):
        return 0 if which < GATE else 1 + 2 * t + which

    def load(s, which, t):
        src = raw(me.half, which, t) if s == OWN else given(KIND_OF[s], which, t)
        return local(src, at_slot(s, which, t), ld.at[s, sem(which, t)])

    def came(kind, t):
        return not first and (t is None or (isinstance(t, int) and (t < AHEAD[kind] or (kind == S and t == EARLY))))

    def move(kind, which, t):
        n = sem(which, t)
        sems = (y_s.at[kind, n], y_r.at[kind, n])
        if kind == S:
            return remote(raw(me.half, which, t), at_slot(MATE, which, t), *sems, me.mate)
        if kind == T:
            return remote(raw(1 - me.half, which, t), at_slot(PART, which, t), *sems, me.partner)
        src = given(T, which, t) if came(T, None if which < GATE else t) else at_slot(PART, which, t)
        return remote(src, at_slot(FAR, which, t), *sems, me.mate)

    def parts(t):
        return [(GATE - 1, 0)] if t is None else [(w, t) for w in GU]

    def send(kind, *ts):
        for t in ts:
            for p in parts(t):
                move(kind, *p).start()

    @timed('relay')
    def relay(*ts):
        for t in ts:
            for p in parts(t):
                if not came(T, t):
                    move(T, *p).wait_recv()
                move(F, *p).start()

    @timed('have')
    def have(*ts):
        for t in ts:
            for p in parts(t):
                load(OWN, *p).wait()
                if came(S, t):
                    load(MATE, *p).wait()
                else:
                    move(S, *p).wait_recv()
                if came(T, t):
                    load(PART, *p).wait()
                if came(F, t):
                    load(FAR, *p).wait()
                else:
                    move(F, *p).wait_recv()

    every = [None, *range(NT)]
    for t in every:
        for p in parts(t):
            load(OWN, *p).start()
            for s, kind in KIND_OF.items():
                if came(kind, t):
                    load(s, *p).start()

    with scope('meet'):
        me.meet(me.sib, me.next, me.prev, me.mate, me.partner, *([me.across] if first else []))

    own_o, oth_o = out_rows(layer, me.half, wo, wd), out_rows(layer, 1 - me.half, wo, wd)
    no = wo.shape[1] // 2
    ahead_o = zip(oth_o + [own_o[0], own_o[1].at[pl.ds(0, s_o.shape[0] - no), :]], split_rows(t_o, no) + split_rows(s_o, no),
                  [me.partner, me.partner, me.mate, me.mate])
    out_moves = [remote(src, dst, o_s.at[n], o_r.at[n], dev) for n, (src, dst, dev) in enumerate(ahead_o)]

    if first:
        then = Place(chips, layer + 1)
        pn = Pieces(layer + 1, wq, wg, wu, then)
        out_moves += [remote(pn.g(then.half, which, EARLY), pc.tile_part(sg1, which), o_s.at[4 + which], o_r.at[4 + which], then.mate) for which in GU]

    small = []
    if first:
        kv_own = local(wkv.at[:, span(me.j, wkv.shape[1] // mp), :], wkvp.at[:, OWN], own_sem.at[4])
        kv_own.start()
        for s, dev in ((PART, me.partner), (MATE, me.mate), (FAR, me.across)):
            small.append(remote(gam, gb.at[s], ex_s.at[s], ex_r.at[s], dev))
        for s, dev in ((PART, me.partner), (MATE, me.mate)):
            small.append(remote(lens, lenb.at[s], ex_s.at[7 + s], ex_r.at[7 + s], dev))
        for c in small:
            c.start()
        gb[OWN] = gam[:, :]
        lenb[OWN] = lens[:, :]
        kv_own.wait()

        def kv_move(kind):
            src, dst, dev = ((OWN, MATE, me.mate), (OWN, PART, me.partner), (PART, FAR, me.mate))[kind]
            return remote(wkvp.at[:, src], wkvp.at[:, dst], ex_s.at[4 + kind], ex_r.at[4 + kind], dev)
        for k in (T, S):
            kv_move(k).start()
            send(k, 0)
        with scope('small'):
            for c in small:
                c.wait_recv()
    else:
        relay(1)
        send(S, 2, 3)

    @timed('norm')
    def norm():
        rb = 32

        @each(0, tok // rb)
        def _(i):
            rows = span(i, rb)
            xf = x[rows, :].astype(F32)
            mu = jnp.mean(xf, axis=-1, keepdims=True)
            xc = xf - mu
            rstd = lax.rsqrt(jnp.mean(xc * xc, axis=-1, keepdims=True) + EPS)
            for s in SLOTS:
                cols = span(me.slots[s], d4)
                hown[rows, cols] = ((x[rows, cols].astype(F32) - mu) * rstd * gb[me.named[s], layer:layer + 1, :]).astype(BF)
    norm()

    SIB, TO, SHARE, PASS, LAST = range(5)

    def gather(g, src, block, part):
        offs = (chips - 1, 1)
        dirs = (me.next, me.prev)

        def idx(off):
            return me.chip_at(off) * 2 + me.core

        def c(kind, k, h):
            n = 4 * kind + 2 * k + h
            sems = (ag_s.at[g, n], ag_r.at[g, n])
            if kind == SIB:
                return remote(src, block(me.j), *sems, me.sib)
            if kind == TO:
                return remote(part(src, h), part(block(me.j), h), *sems, dirs[k])
            b = part(block(idx(2 if kind == LAST else offs[k])), h)
            return remote(b, b, *sems, dirs[k] if kind == PASS else me.sib)

        mine = local(src, block(me.j), own_sem.at[g])
        tag = 'abvw'[g]

        class G:
            @timed('own' + tag)
            def own():
                for h in range(2):
                    for k in range(2):
                        c(TO, k, k ^ h).start()
                c(SIB, 0, 0).start()
                mine.start()

            @timed('near' + tag)
            def near():
                for h in range(2):
                    for k in range(2):
                        c(TO, k, k ^ h).wait_recv()
                        if h == 0:
                            c(PASS, k, k).start()
                        c(SHARE, k, k ^ h).start()

            @timed('far' + tag)
            def far():
                for k in range(2):
                    c(PASS, k, k).wait_recv()
                    c(LAST, k, k).start()

            @timed('has' + tag)
            def has(kind):
                if kind == SIB:
                    mine.wait()
                    c(SIB, 0, 0).wait_recv()
                for k in range(2):
                    if kind == LAST:
                        c(kind, k, k).wait_recv()
                    if kind == SHARE:
                        for h in range(2):
                            c(kind, k, k ^ h).wait_recv()

            def end():
                c(SIB, 0, 0).wait_send()
                for k in range(2):
                    for h in range(2):
                        c(TO, k, h).wait_send()
                        c(SHARE, k, h).wait_send()
                    c(PASS, k, k).wait_send()
                    c(LAST, k, k).wait_send()
        return G

    def h_block(b):
        return lambda j: hbuf.at[b, span(j, tok), :]

    def h_part(ref, k):
        return ref.at[pl.ds(k * (tok // 2), tok // 2), :]

    ga, gb2 = gather(0, hown, h_block(MINE), h_part), gather(1, hpar, h_block(THEIRS), h_part)
    ht = remote(hown, hpar, ex_s.at[7], ex_r.at[7], me.partner)

    rows2 = 2 * tok

    def chip_rows(i):
        return span(me.chip_at(i + i // 2 - 2 * (i // 3)), rows2)

    def hload(i):
        return local(hbuf.at[i // chips, chip_rows(lax.rem(i, chips)), :], hv.at[lax.rem(i, 2), pl.ds(0, rows2), :], hv_sem.at[lax.rem(i, 2)])

    def hdot(i, rows, w):
        acc = None
        for s in SLOTS:
            p = dot(hv[lax.rem(i, 2), :rows, span(me.slots[s], d4)], w(s))
            acc = p if acc is None else acc + p
        return acc

    def mcopy(b, rows, n, t, k):
        w = pc.tile
        return local(ms.at[k, pl.ds(0, n), :], om.at[b, rows, pl.ds(pl.multiple_of(nq + t * w, w), w)], ms_sem.at[k])

    def tile(i, b, rows, n, t, m):
        k = lax.rem(m, 2)
        a = hdot(i, n, lambda s: wgu[s, t])

        @pl.when(m >= 2)
        def _():
            mcopy(b, rows, n, t, k).wait()
        gt = a[:, :pc.tile].astype(BF).astype(F32)
        up = a[:, pc.tile:].astype(BF).astype(F32)
        ms[k, :n, :] = (gt * jax.nn.sigmoid(gt) * up).astype(BF)
        mcopy(b, rows, n, t, k).start()

    def drain(n):
        for k in range(2):
            mcopy(MINE, pl.ds(0, n), n, 0, k).wait()

    def any_of(i, marks):
        return functools.reduce(lambda a, b: a | b, [i == g for g in marks])

    def sweep(b, qk, nt, gates, hooks):
        lo = b * chips
        marks = [n for n in gates]

        @each(lo, lo + chips)
        def _(i):
            for g, f in gates.items():
                pl.when(i == g)(f)

            @pl.when(any_of(i, [lo, *marks]))
            def _():
                hload(i).start()

            @pl.when(jnp.logical_not(any_of(i + 1, [lo + chips, *marks])))
            def _():
                hload(i + 1).start()
            hload(i).wait()
            rows = chip_rows(i - lo)
            if qk:
                qkv[b, rows, :] = hdot(i, rows2, lambda s: wqkv[s]).astype(BF)

            @each(0, nt)
            def _(t):
                for n, f in hooks.items():
                    pl.when((i == lo) & (b == MINE) & (t == n))(f)
                tile(i, b, rows, rows2, t, (i - lo) * nt + t)

        @pl.when(nt + lo >= 1)
        def _():
            drain(rows2)

    def late(lo_t, hi_t, lo, hi, hooks):
        big = hv.shape[1]
        per = qkv.shape[1] // big
        n = (hi - lo) * per

        def place(u):
            v = lo * per + lax.rem(u, n)
            return v // per, span(lax.rem(v, per), big)

        def load_big(u):
            b, rows = place(u)
            return local(hbuf.at[b, rows, :], hv.at[lax.rem(u, 2)], hv_sem.at[lax.rem(u, 2)])

        def run():
          @each(0, n * (hi_t - lo_t))
          def _(u):
            t = lo_t if hi_t - lo_t == 1 else lo_t + u // n

            @pl.when(lax.rem(u, n) == 0)
            def _():
                have(t)
            for k, f in hooks.items():
                pl.when(u == k)(f)

            @pl.when(u + 1 < n * (hi_t - lo_t))
            def _():
                load_big(u + 1).start()
            load_big(u).wait()
            b, rows = place(u)
            tile(u, b, rows, big, t, u)
          drain(big)
        return load_big(0).start, run

    bq, bk = sc.shape[1:]

    @timed('attend')
    def attend(b):
        nblk = qkv.shape[1] // bq
        ratio = bk // bq

        def ocp(i, k):
            return local(os.at[k], om.at[b, span(i, bq), pl.ds(0, dh)], os_sem.at[k])

        def lanes(a, op):
            return functools.reduce(op, [a[:, n * LANES:(n + 1) * LANES] for n in range(bk // LANES)])

        @each(0, nblk)
        def _(i):
            q = qkv[b, span(i, bq), pl.ds(0, dh)]
            length = lenb[b * me.named[PART], :, :][:1, :1]
            colf = lax.broadcasted_iota(jnp.int32, (1, bk), 1).astype(F32)

            def raw_score(j):
                k = qkv[b, span(j, bk), pl.ds(dh, dh)]
                s = lax.dot_general(q, k, (((1,), (1,)), ((), ())), preferred_element_type=F32) * (dh ** -0.5)
                pos = jnp.broadcast_to(colf + (j * bk).astype(F32), (bq, bk))
                return jnp.where(pos < length, s, -1e30)

            def score(j, m):
                s = raw_score(j)
                sc[j] = s
                return jnp.maximum(m, lanes(s, jnp.maximum))

            last = i // ratio
            row = lax.broadcasted_iota(jnp.int32, (bq, bk), 0) + (i - last * ratio) * bq
            col = lax.broadcasted_iota(jnp.int32, (bq, bk), 1)
            s = jnp.where(col <= row, raw_score(last), -1e30)
            sc[last] = s
            m = jnp.max(lax.fori_loop(0, last, score, lanes(s, jnp.maximum)), axis=1, keepdims=True)

            def expo(j, l):
                p = jnp.exp(sc[j] - m)
                sc[j] = p
                return l + lanes(p, jnp.add)

            l = jnp.sum(lax.fori_loop(0, last + 1, expo, jnp.zeros((bq, LANES), F32)), axis=1, keepdims=True)
            inv = 1.0 / l

            def value(j, o):
                return o + dot((sc[j] * inv).astype(BF), qkv[b, span(j, bk), pl.ds(2 * dh, dh)])

            o = lax.fori_loop(0, last + 1, value, jnp.zeros((bq, dh), F32))
            k = lax.rem(i, 2)

            @pl.when(i >= 2)
            def _():
                ocp(i, k).wait()
            os[k] = o.astype(BF)
            ocp(i, k).start()
        for k in range(2):
            ocp(k, k).wait()

    def kv_load(u):
        s, j = u // mp, lax.rem(u, mp)
        name = s if first else s + (1 - s // 3) * (s - s // 2 * 2 - s // 2 * 1)
        return local(wkvb.at[layer, j, s], wqkv.at[name, span(j, wkvp.shape[2]), pl.ds(nq, 2 * dh)], kv_sem.at[u])

    def kv_loads(go):
        @each(0, 4 * mp)
        def _(u):
            go(kv_load(u))

    def near_of(g):
        def f():
            g.near()
            g.has(SHARE)
        return f

    def far_of(g):
        def f():
            g.far()
            g.has(LAST)
        return f

    def both(*fs):
        def f():
            for g in fs:
                g()
        return f

    def start_b():
        with scope('ht'):
            ht.wait_recv()
        gb2.own()

    ga.own()
    if first:
        with scope('kvmove'):
            kv_move(T).wait_recv()
            kv_move(F).start()
        send(T, None)
        with scope('kvmove2'):
            kv_move(S).wait_recv()
            kv_move(F).wait_recv()
        gw = [gather(2 + n, wkvp.at[n], lambda j, n=n: wkvb.at[n, j], lambda ref, k: ref.at[pl.ds(2 * k, 2)]) for n in range(2)]
        relay(0)
        send(S, None)
        ht.start()
        relay(None)
        ga.near()
        gw[0].own()
        for kind in (SIB, SHARE):
            ga.has(kind)
        have(0)
        send(S, 1)
        send(T, 1)
        send(S, 2)

        def far_a():
            ga.far()
            ga.has(LAST)
        with scope('pre'):
            sweep(MINE, False, 1, {3: far_a}, {})
        gw[0].near()
        start_b()
        send(T, 2)
        send(T, 3)
        gw[0].far()
        for c in out_moves[:2]:
            c.start()
        for kind in (SIB, SHARE, LAST):
            gw[0].has(kind)
        kv_loads(lambda c: c.start())
        kv_loads(lambda c: c.wait())
        have(None)
        load_late, run_late = late(1, NT, MINE, len(SEQS), {4: gw[1].near, 8: gw[1].far})

        @each(0, 2)
        def _(b):
            with scope('sweep'):
                sweep(b, True, b, {chips: both(lambda: gb2.has(SIB), gb2.near), chips + 1: both(lambda: gb2.has(SHARE), lambda: relay(2)),
                                   chips + 3: far_of(gb2)}, {})

            @pl.when(b == MINE)
            def _():
                relay(1)
                send(S, 3)

            @pl.when(b == THEIRS)
            def _():
                relay(3)
                for c in out_moves[2:]:
                    c.start()
                gw[1].own()
                load_late()
            attend(b)

        with scope('late'):
            run_late()
        for kind in (SIB, SHARE, LAST):
            gw[1].has(kind)
    else:
        ht.start()
        send(T, 2, 3)
        for c in out_moves[:2]:
            c.start()
        kv_loads(lambda c: c.start())
        kv_loads(lambda c: c.wait())
        have(None, 0)

        def far_a():
            far_of(ga)()
            relay(2)
        load_some, run_some = late(2, 3, MINE, THEIRS, {})
        load_late, run_late = late(3, NT, MINE, len(SEQS), {})

        @each(0, 2)
        def _(b):
            with scope('sweep'):
                sweep(b, True, 2 + b, {0: lambda: ga.has(SIB), 1: both(near_of(ga), start_b), 3: far_a,
                                       chips: both(lambda: gb2.has(SIB), gb2.near), chips + 1: lambda: gb2.has(SHARE), chips + 3: far_of(gb2)},
                      {1: lambda: have(1)})
            pl.when(b == MINE)(load_some)
            pl.when(b == THEIRS)(load_late)
            attend(b)

            @pl.when(b == MINE)
            def _():
                relay(3)
                for c in out_moves[2:]:
                    c.start()
                with scope('late2'):
                    run_some()
        with scope('late'):
            run_late()

    with scope('end'):
        for t in every:
            for p in parts(t):
                for k in KINDS:
                    if not came(k, t):
                        move(k, *p).wait_send()
        for c in out_moves:
            c.wait()
        ht.wait_send()
        ga.end()
        gb2.end()
        for c in small:
            c.wait_send()
        if first:
            gw[0].end()
            gw[1].end()
            for k in KINDS:
                kv_move(k).wait_send()


EARLY = 1
AHEAD = (1, 2, 1)


def front(layer, mesh, x, gam, lens, weights, given):
    wq, wkv, wg, wu, wo, wd = weights
    tok, d = x.shape
    mp = mesh.shape['mp']
    chips = mp // 2
    first = layer == 0
    d4 = wq.shape[1]
    nq, nkv, nf = wq.shape[2] // 2, wkv.shape[2], wg.shape[2] // 2
    no, nd = wo.shape[1] // 2, wd.shape[1] // 2
    t = tok * mp
    kvr = wkv.shape[1] // mp
    sds = jax.ShapeDtypeStruct
    outs = [sds((2, t, nq + nf), BF), sds((2, t, d), BF), sds((no + (nd // 4 if first else nd), d4), BF), sds((no + nd, d4), BF)]
    specs = [ANY] * 4
    if first:
        outs += [sds((d4, 2 * nf // NT), BF), sds((2, mp, 4, kvr, nkv), BF), sds((4, *gam.shape), F32), sds((3, *lens.shape), F32)]
        specs += [ANY, ANY, VM, VM]
    npiece = 1 + 2 * NT
    return pl.pallas_call(
        functools.partial(front_kernel, layer, chips), out_shape=outs,
        in_specs=[VM, VM, VM] + [ANY] * (6 + len(given)), out_specs=specs,
        scratch_shapes=[
            pltpu.VMEM((4, d4, nq + nkv), BF), pltpu.VMEM((4, NT, d4, 2 * nf // NT), BF), pltpu.VMEM((2, 4 * tok, d), BF),
            pltpu.VMEM((2, t, nq + nkv), BF), pltpu.VMEM((tok, d), BF), pltpu.VMEM((tok, d), BF),
            pltpu.VMEM((2, 4, kvr, nkv), BF), pltpu.VMEM((t // BLOCK, BLOCK, BLOCK), F32),
            pltpu.VMEM((2, 4 * tok, nf // NT), BF), pltpu.VMEM((2, BLOCK, nq), BF),
            DMA((3, npiece)), DMA((3, npiece)), DMA((4, npiece)), DMA((6,)), DMA((6,)), DMA((4 * mp,)), DMA((2,)), DMA((2,)), DMA((2,)),
            DMA((4, 20)), DMA((4, 20)), DMA((5,)), DMA((10,)), DMA((10,))],
        compiler_params=pltpu.CompilerParams(vmem_limit_bytes=VMEM_LIMIT, collective_id=2 * layer, has_side_effects=True),
        cost_estimate=pl.CostEstimate(flops=4 * t * d * (nq + nkv + 2 * nf), bytes_accessed=12 * t * d, transcendentals=0),
        name=f"front{layer}")(x, gam, lens, *weights, *given)


def back_kernel(layer, chips, nxt, *refs):
    it = iter(refs)
    take = lambda n: [next(it) for _ in range(n)]
    x, om_h, s_o, t_o, wo, wd = take(6)
    if nxt:
        wq, wg, wu = take(3)
    y = next(it)
    if nxt:
        bufs = take(6)
    (om, w, sl, rel, fin, zt, sib, acc, in_sem, w_s, w_r, p_s, p_r, sib_s, sib_r, rel_s, rel_r, fin_s, fin_r, t_s, t_r) = it
    me = Place(chips, layer)
    nb, rows = zt.shape[:2]
    per = w.shape[2] // CB
    no, ns = wo.shape[1] // 2, s_o.shape[0]

    own_o = out_rows(layer, me.half, wo, wd)
    own_rows, mate_rows = split_rows(w.at[OWN], no), split_rows(w.at[MATE], ns)
    loads = [local(om_h.at[THEIRS], om.at[THEIRS], in_sem.at[0]), local(own_o[0], own_rows[0], in_sem.at[1]),
             local(own_o[1], own_rows[1], in_sem.at[2]), local(t_o, w.at[PART], in_sem.at[3]), local(om_h.at[MINE], om.at[MINE], in_sem.at[4]),
             local(s_o, mate_rows[0], in_sem.at[5])]
    for c in loads[:3]:
        c.start()
    me.meet(me.sib, me.next, me.prev, me.mate, me.partner)
    for c in loads[3:]:
        c.start()
    to_mate = [remote(t_o.at[:, span(n, CB)], w.at[FAR, :, span(n, CB)], w_s.at[n], w_r.at[n], me.mate) for n in range(per)]
    if nxt:
        to_mate.insert(0, remote(own_o[1].at[pl.ds(ns - no, no + own_o[1].shape[0] - ns), :], mate_rows[1], w_s.at[per], w_r.at[per], me.mate))
    else:
        for c in to_mate:
            c.start()
    passing = []
    if nxt:
        then = Place(chips, layer + 1)
        pc = Pieces(layer + 1, wq, wg, wu, then)

        def ahead(kind, dev):
            q, g = bufs[2 * kind:2 * kind + 2]
            dst = [q] + [pc.tile_part(g.at[t], which) for t in range(AHEAD[kind]) for which in GU]
            if kind == F:
                q, g = bufs[2 * T:2 * T + 2]
                src = [q] + [pc.tile_part(g.at[t], which) for t in range(AHEAD[F]) for which in GU]
            else:
                half = then.half if kind == S else 1 - then.half
                src = [pc.q(half)] + [pc.g(half, which, t) for t in range(AHEAD[kind]) for which in GU]
            return [remote(*sd, p_s.at[kind, n], p_r.at[kind, n], dev) for n, sd in enumerate(zip(src, dst))]
        to_s, to_t, on = ahead(S, then.mate), ahead(T, then.partner), ahead(F, then.mate)
        for c in (*to_t[:len(on)], *to_mate, *to_s, *to_t[len(on):]):
            c.start()
        passing = to_s + on + to_t[len(on):]
    with scope('loads'):
        for c in loads[:4]:
            c.wait()

    AWAY, NEAR, JOIN, HOME = range(4)

    def sib_copy(st, b, cb, m):
        k = lax.rem(m, RING)
        return remote(sib.at[k], sl.at[st, b, cb], sib_s.at[k], sib_r.at[st, b, cb], me.sib)

    def away_copy(b, cb):
        return remote(sl.at[AWAY, b, cb], rel.at[b, cb], rel_s.at[b, cb], rel_r.at[b, cb], me.at(1 + 2 * lax.rem(cb, 2)))

    def near_copy(st, b, cb):
        p = lax.rem(st + cb, 2)
        return remote(sl.at[st, b, cb], fin.at[p, b, cb], fin_s.at[p, b, cb], fin_r.at[p, b, cb], me.at(1 + 2 * p))

    def compute(off, st, b, cb, m):
        a = acc.at[lax.rem(m, LAG + 1)]
        a[:, :] = dot(om[b, span(me.chip_at(off), 2 * rows), :], w[cb // per, :, span(lax.rem(cb, per), CB)])

        @pl.when(m >= RING)
        def _():
            sib_copy(st, b, cb, m).wait_send()
        sib[lax.rem(m, RING)] = a[span(1 - me.core, rows), :].astype(BF)
        sib_copy(st, b, cb, m).start()

    def combined(st, b, cb, m):
        sib_copy(st, b, cb, m).wait_recv()
        a = acc.at[lax.rem(m, LAG + 1)]
        return a[span(me.core, rows), :] + sl[st, b, cb].astype(F32)

    def run(n, unit, off, finish):
        @each(0, n + LAG)
        def _(m):
            @pl.when(m < n)
            def _():
                st, b, cb = unit(m)
                compute(off(st, cb), st, b, cb, m)

            @pl.when(m >= LAG)
            def _():
                st, b, cb = unit(m - LAG)
                finish(st, b, cb, combined(st, b, cb, m - LAG))

        for m in range(RING):
            @pl.when(m < n)
            def _(m=m):
                sib_copy(HOME, MINE, 0, m).wait_send()

    @timed('depart')
    def depart(lo, n):
        def unit(m):
            return m // (2 * n), 1 - lax.rem(m // n, 2), lo + lax.rem(m, n)

        def off(st, cb):
            return (1 - st) * 2 + st * (1 + 2 * lax.rem(st + cb, 2))

        def on(st, b, cb, v):
            sl[st, b, cb] = v.astype(BF)

            @pl.when(st == AWAY)
            def _():
                away_copy(b, cb).start()

            @pl.when(st == NEAR)
            def _():
                near_copy(NEAR, b, cb).start()
        run(4 * n, unit, off, on)

    @timed('join')
    def join(lo, n):
        def unit(m):
            return JOIN + m // (2 * n), 1 - lax.rem(m // n, 2), lo + lax.rem(m, n)

        def off(st, cb):
            return (HOME - st) * (1 + 2 * lax.rem(st + cb, 2))

        def on(st, b, cb, v):
            @pl.when(st == JOIN)
            def _():
                away_copy(b, cb).wait_recv()
                sl[JOIN, b, cb] = (v + rel[b, cb].astype(F32)).astype(BF)
                near_copy(JOIN, b, cb).start()

            @pl.when(st == HOME)
            def _():
                sl[HOME, b, cb] = v.astype(BF)
        run(4 * n, unit, off, on)

    def t_copy(cb):
        return remote(sl.at[HOME, THEIRS, cb], zt.at[cb], t_s.at[cb], t_r.at[cb], me.partner)

    def total(b, cb):
        for p in range(2):
            local(fin.at[p, b, cb], fin.at[p, b, cb], fin_r.at[p, b, cb]).wait()
        return sl[HOME, b, cb].astype(F32) + fin[0, b, cb].astype(F32) + fin[1, b, cb].astype(F32)

    @timed('theirs')
    def theirs(lo, hi):
        @each(lo, hi)
        def _(cb):
            sl[HOME, THEIRS, cb] = total(THEIRS, cb).astype(BF)
            t_copy(cb).start()

    def swapped(cb):
        slot = cb // per
        return (slot + 1 - 2 * (slot % 2)) * per + cb % per

    def give_copy(st, cb):
        if st == HOME:
            return t_copy(cb)
        if st == AWAY:
            dst, *sems = rel.at[THEIRS, cb], rel_s.at[THEIRS, cb], rel_r.at[THEIRS, cb]
        else:
            p = st - NEAR
            dst, *sems = fin.at[p, THEIRS, cb], fin_s.at[p, THEIRS, cb], fin_r.at[p, THEIRS, cb]
        return remote(sl.at[st, THEIRS, cb], dst, *sems, me.partner)

    def given(st, cb):
        c = swapped(cb)
        give_copy(st, c).wait_recv()
        return (rel[THEIRS, c] if st == AWAY else zt[c] if st == HOME else fin[st - NEAR, THEIRS, c]).astype(F32)

    def offset(st, cb):
        first, home = (HOME - st) // HOME, st // HOME
        return 2 * first + (1 - first) * (1 - home) * (1 + 2 * lax.rem(st + cb, 2))

    @timed('give')
    def give(lo, n):
        def unit(m):
            return lax.rem(m, 4), THEIRS, swapped(lo + m // 4)

        def on(st, b, cb, v):
            sl[st, THEIRS, cb] = v.astype(BF)
            for k in (AWAY, NEAR, JOIN, HOME):
                @pl.when(st == k)
                def _(k=k):
                    give_copy(k, cb).start()
        run(4 * n, unit, offset, on)

    @timed('take')
    def take(lo, n):
        def unit(m):
            k = lax.rem(m, 4)
            return k + k // 2 - 2 * (k // 3), MINE, lo + m // 4

        def on(st, b, cb, v):
            for k in (AWAY, NEAR, JOIN, HOME):
                @pl.when(st == k)
                def _(k=k):
                    z = v + given(k, cb)
                    if k == JOIN:
                        away_copy(MINE, cb).wait_recv()
                        z = z + rel[MINE, cb].astype(F32)
                    sl[k, MINE, cb] = z.astype(BF)
                    if k == AWAY:
                        away_copy(MINE, cb).start()
                    elif k != HOME:
                        near_copy(k, MINE, cb).start()
        run(4 * n, unit, offset, on)

    @timed('mine')
    def mine(slot, with_theirs):
        @each(0, per)
        def _(n):
            cb = slot * per + n
            z = total(MINE, cb)
            if with_theirs:
                t_copy(swapped(cb)).wait_recv()
                z = z.astype(BF).astype(F32) + zt[swapped(cb)].astype(F32)
            cols = span(me.slots[slot] * per + n, CB)
            y[:, cols] = (x[:, cols].astype(F32) + z).astype(BF)

    def wait_rest():
        loads[4].wait()
        loads[5].wait()

    if nxt:
        @each(0, 4)
        def _(g):
            n = 2 * per // (1 + g)
            lo = nb - 2 * n + g // 3
            pl.when(g == 0)(wait_rest)
            for k in range(len(to_mate)):
                @pl.when(g == 1 + k)
                def _(k=k):
                    with scope('w%d' % k):
                        to_mate[k].wait_recv()
            depart(lo, n)

            @pl.when(g == 0)
            def _():
                join(lo, n)
                with scope('passing'):
                    for t, f in zip(to_t, on):
                        t.wait_recv()
                        f.start()

            @pl.when(g == 1)
            def _():
                theirs(0, 2 * per)

            @pl.when(g == 2)
            def _():
                join(2 * per, per)
                theirs(2 * per, 3 * per)
        join(3 * per, per)
        theirs(3 * per, nb)
    else:
        @each(0, 2)
        def _(g):
            give(g, 1 + 2 * g)

            @pl.when(g == 0)
            def _():
                wait_rest()

            @pl.when(g == 1)
            def _():
                take(per * OWN, per)
                theirs(per * MATE, per * FAR)
                with scope('w'):
                    for c in to_mate:
                        c.wait_recv()
            depart(per * (MATE + g), per)
            join(per * (MATE + g), per)
        take(per * PART, per)
        theirs(per * FAR, nb)
    for slot in SLOTS:
        mine(slot, nxt or slot in (MATE, FAR))

    with scope('end'):
        @each(0, nb)
        def _(cb):
            t_copy(cb).wait_send()
            for b in SEQS:
                away_copy(b, cb).wait_send()
                for st in (NEAR, JOIN):
                    near_copy(st, b, cb).wait_send()
        for c in to_mate:
            c.wait_send()
        for c in passing:
            c.wait()
        if nxt:
            for c in to_t[:len(on)]:
                c.wait_send()


def back(layer, mesh, x, om, s_o, t_o, weights, last):
    wq, wkv, wg, wu, wo, wd = weights
    mp = mesh.shape['mp']
    tok, d = x.shape
    t, k = om.shape[1:]
    d4 = wo.shape[2]
    nb = d // CB
    unit = (tok, CB)
    nq, nf = wq.shape[2] // 2, wg.shape[2] // 2
    sds = jax.ShapeDtypeStruct
    outs, specs = [sds((tok, d), BF)], [VM]
    args = [x, om, s_o, t_o, wo, wd]
    if not last:
        args += [wq, wg, wu]
        for n in AHEAD:
            outs += [sds((d4, nq), BF), sds((n, d4, 2 * nf // NT), BF)]
        specs += [ANY] * 6
    npiece = 1 + 2 * NT
    return pl.pallas_call(
        functools.partial(back_kernel, layer, mp // 2, not last), out_shape=outs,
        in_specs=[VM] + [ANY] * (len(args) - 1), out_specs=specs,
        scratch_shapes=[
            pltpu.VMEM((2, t, k), BF), pltpu.VMEM((4, k, d4), BF),
            pltpu.VMEM((4, 2, nb, *unit), BF), pltpu.VMEM((2, nb, *unit), BF), pltpu.VMEM((2, 2, nb, *unit), BF), pltpu.VMEM((nb, *unit), BF),
            pltpu.VMEM((RING, *unit), BF), pltpu.VMEM((LAG + 1, 2 * tok, CB), F32),
            DMA((6,)), DMA((3,)), DMA((3,)), DMA((3, npiece)), DMA((3, npiece)), DMA((RING,)), DMA((4, 2, nb)),
            DMA((2, nb)), DMA((2, nb)), DMA((2, 2, nb)), DMA((2, 2, nb)), DMA((nb,)), DMA((nb,))],
        compiler_params=pltpu.CompilerParams(vmem_limit_bytes=VMEM_LIMIT, collective_id=2 * layer + 1, has_side_effects=True),
        cost_estimate=pl.CostEstimate(flops=4 * t * k * d, bytes_accessed=2 * (2 * t * k + 4 * k * d4), transcendentals=0),
        name=f"back{layer}")(*args)


def solution(mesh):
    assert mesh.shape['dp'] == len(SLOTS)

    def body(x, lengths, gamma, *weights):
        layers = gamma.shape[0]
        assert layers == 2
        x = x[0]
        gam = jnp.zeros((8, gamma.shape[1]), F32).at[:layers].set(gamma.astype(F32))
        lens = jnp.broadcast_to(lengths.astype(F32)[:, None], (8, 128))
        om, _, s_o, t_o, sg1, wkvb, gam, lens = front(0, mesh, x, gam, lens, weights, ())
        x, *ahead = back(0, mesh, x, om, s_o, t_o, weights, False)
        om, _, s_o, t_o = front(1, mesh, x, gam, lens, weights, (sg1, wkvb, *ahead))
        (x,) = back(1, mesh, x, om, s_o, t_o, weights, True)
        return x[None]

    in_specs = (P(('rep', 'dp'), 'mp', None), P(('rep', 'dp')), P(None, 'dp'),
                P(None, 'dp', 'mp'), P(None, 'dp', None), P(None, 'dp', 'mp'),
                P(None, 'dp', 'mp'), P(None, 'mp', 'dp'), P(None, 'mp', 'dp'))
    return jax.shard_map(body, mesh=mesh, in_specs=in_specs,
                         out_specs=P(('rep', 'dp'), 'mp', None), check_vma=False)
```
